128 devices in a mesh: act: 4 (over y), virt: 32 (over x, z, core).
Axes of the slice: x: 4, y: 4, z: 4, core: 2. Of those that a mesh axis runs over, the one named last changes fastest.
Arguments:
- amplitudes: bfloat16 [400, 640, 640], P('act', 'virt'), may hold values from -6 to 6
- virtual_fock_block: bfloat16 [640, 640], replicated, may hold values from -1 to 3.1, as said below
- metric: bfloat16 [400, 400], replicated, may hold values from -3.5 to 3.5, as said below
- active_block: bfloat16 [400, 400], replicated, may hold values from -0.3125 to 0.3125
Outputs:
- residual_vec: bfloat16 [400, 640, 640], P('act', 'virt')
- rayleigh: float32 [], replicated
- res_norm: float32 [], replicated
The draws below stay inside these ranges and needn't reach their ends.
Inputs may be any that keep to these rules, and one draw needn't show every extreme that they name: `virtual_fock_block`: symmetric. `metric`: symmetric positive definite.
All inputs are finite; a program needn't handle non-finite values.
Results may differ from the reference program's by a relative error of at most 0.0099.
Values may be sent and summed in bfloat16 or wider, within the bound.
No kernel may reach another device: no remote copies, remote signals or barrier semaphores. Data moves between devices by JAX's collectives and lax.ppermute only.
A program may use at most 128 MiB of HBM per device.

```python
import jax
import jax.numpy as jnp
from jax import lax

NV = 640
TU = 400


def draw_virtual_fock_block(key, part):
    leading_key, second_key = jax.random.split(jax.random.fold_in(key, 11))
    energies = jax.random.uniform(leading_key, (NV,), jnp.float32, 0.5, 3.0)
    coupling = jax.random.uniform(second_key, (NV, NV), jnp.float32, -1.0, 1.0) * 1.7
    coupling = (coupling + coupling.T) * (0.35 / math_sqrt(NV))
    coupling = coupling * (1.0 - jnp.eye(NV, dtype=jnp.float32))
    return (jnp.diag(energies) + coupling).astype(jnp.bfloat16)


def math_sqrt(value):
    return float(value) ** 0.5


def draw_metric(key, part):
    leading_key = jax.random.fold_in(jax.random.fold_in(key, 23), 0)
    factor = jax.random.uniform(leading_key, (TU, TU), jnp.float32, -1.7, 1.7)
    product = jnp.dot(factor, factor.T, precision=lax.Precision.HIGHEST) / TU
    return (0.5 * jnp.eye(TU, dtype=jnp.float32) + product).astype(jnp.bfloat16)


def level_of(own_key, extent, pieces, least, top_value):
    level, own = 1.0, jax.random.fold_in(own_key, 6)
    for axis_at, shards_of in pieces:
        heights = jnp.exp(jax.random.uniform(jax.random.fold_in(own, axis_at), (shards_of,), jnp.float32, least / len(pieces), top_value / len(pieces)))
        level = level * jnp.repeat(heights, extent[axis_at] // shards_of).reshape([-1 if axis == axis_at else 1 for axis in range(len(extent))])
    return level


def noise(key, shape, scale, most, shards=(), held_as=jnp.bfloat16):
    drawn = jax.random.normal(key, shape, jnp.float32) * scale
    if len(shards) > 0:
        drawn = level_of(key, shape, shards, -0.22, 0.18) * drawn
    return jnp.clip(drawn, min=-most, max=most).astype(held_as)


def setup_inputs(seed: int = 0) -> dict:
    keys = jax.random.split(jax.random.key(seed), 5)
    amplitudes = noise(keys[0], (TU, NV, NV), 1.0, 6.0, ((0, 4), (1, 32)))
    virtual_fock_block = draw_virtual_fock_block(jax.random.fold_in(keys[4], 71), 0)
    metric = draw_metric(jax.random.fold_in(keys[4], 71), 0)
    active_block = noise(keys[3], (TU, TU), TU ** -0.5, 0.3125)
    return dict(amplitudes=amplitudes, virtual_fock_block=virtual_fock_block, metric=metric, active_block=active_block)


def reference(amplitudes, virtual_fock_block, metric, active_block):
    broadened_fock = virtual_fock_block.astype(jnp.float32)
    block_of_rows = 32
    blocks_count = NV // block_of_rows
    indices = jnp.arange(blocks_count, dtype=jnp.int32)

    def metric_rows(index):
        start = (index * block_of_rows).astype(jnp.int32)
        trial_rows = lax.dynamic_slice_in_dim(amplitudes, start, block_of_rows, 1)
        flat_trial = trial_rows.reshape(TU, block_of_rows * NV)
        weighted_rows = jnp.dot(metric, flat_trial, preferred_element_type=jnp.float32)
        return weighted_rows.astype(jnp.bfloat16).reshape(TU, block_of_rows, NV)

    half_blocks = lax.map(metric_rows, indices)
    weighted_half = jnp.moveaxis(half_blocks, 0, 1).reshape(TU, NV, NV)

    def left_group(group_rows):
        return jnp.einsum("ac,tcb->tab", broadened_fock, group_rows.astype(jnp.float32)).astype(jnp.bfloat16)

    left_portion = lax.map(left_group, weighted_half.reshape(TU // 4, 4, NV, NV)).reshape(TU, NV, NV)

    def project(index):
        start = (index * block_of_rows).astype(jnp.int32)
        trial_rows = lax.dynamic_slice_in_dim(amplitudes, start, block_of_rows, 1)
        halved_rows = lax.dynamic_slice_in_dim(weighted_half, start, block_of_rows, 1)
        left_rows = lax.dynamic_slice_in_dim(left_portion, start, block_of_rows, 1)
        flat_trial = trial_rows.reshape(TU, block_of_rows * NV)
        rightside_rows = jnp.einsum("wuv,vq->wuq", halved_rows.astype(jnp.float32), broadened_fock)
        sigma_rows = left_rows.astype(jnp.float32).reshape(TU, block_of_rows * NV) + rightside_rows.reshape(TU, block_of_rows * NV) + jnp.dot(active_block, flat_trial, preferred_element_type=jnp.float32)
        weighted_rows = jnp.dot(metric, flat_trial, preferred_element_type=jnp.float32)
        return sigma_rows, weighted_rows, flat_trial.astype(jnp.float32)

    def intersect(index):
        sigma_rows, weighted_rows, trial_wide = project(index)
        return jnp.sum(trial_wide * sigma_rows), jnp.sum(trial_wide * weighted_rows)

    numer_parts, denom_parts = lax.map(intersect, indices)
    numerator = jnp.sum(numer_parts)
    denominator = jnp.sum(denom_parts)
    rayleigh = numerator / denominator

    def finish(index):
        sigma_rows, weighted_rows, trial_wide = project(index)
        resid = sigma_rows - rayleigh * weighted_rows
        return resid.astype(jnp.bfloat16).reshape(TU, block_of_rows, NV), jnp.sum(resid * resid)

    resid_blocks, square_parts = lax.map(finish, indices)
    residual_vec = jnp.moveaxis(resid_blocks, 0, 1).reshape(TU, NV, NV)
    res_norm = jnp.sum(square_parts) / denominator
    return residual_vec, rayleigh, res_norm
```

```python
import functools

import jax
import jax.numpy as jnp
from jax import lax
from jax.experimental import pallas as pl
from jax.experimental.pallas import tpu as pltpu
from jax.sharding import PartitionSpec as P

BF = jnp.bfloat16
F32 = jnp.float32
ALL = ("act", "virt")
LANES = 128
USED = 125
VMEM_LIMIT = 60 * 1024 * 1024
NT_DIMS = (((1,), (1,)), ((), ()))
TN_DIMS = (((0,), (0,)), ((), ()))


def onehot(shape, row_base, column_base, row_end, column_end):
    rows = lax.broadcasted_iota(jnp.int32, shape, 0)
    columns = lax.broadcasted_iota(jnp.int32, shape, 1)
    same = (rows + row_base) == (columns + column_base)
    keep = same & (rows < row_end) & (columns < column_end)
    return jnp.where(keep, 1.0, 0.0).astype(BF)


def touching(pairs, items):
    chunks = pairs * items // USED
    return [
        [i for i in range(items) if i * pairs < (k + 1) * USED and (i + 1) * pairs > k * USED]
        for k in range(chunks)
    ]


def pack_kernel(pitch, x_ref, out_ref, scratch):
    rows, pairs, width = x_ref.shape
    items = width // LANES
    table = touching(pairs, items)
    chunks = len(table)
    sel = {
        (k, i): onehot((pairs, LANES), i * pairs, k * USED, pairs, USED)
        for k in range(chunks)
        for i in table[k]
    }
    for a in range(rows):
        for k in range(chunks):
            total = None
            for i in table[k]:
                part = lax.dot_general(
                    x_ref[a, :, i * LANES : (i + 1) * LANES], sel[k, i], TN_DIMS, preferred_element_type=F32
                )
                total = part if total is None else total + part
            scratch[pl.ds(k * rows + a, LANES, stride=pitch), :] = total
    used = chunks * rows
    for d in range(LANES):
        out_ref[d] = scratch[d * pitch : d * pitch + used, :].astype(BF)


def pack(x):
    rows, pairs, width = x.shape
    used = pairs * (width // LANES) // USED * rows
    pitch = used + 8
    return pl.pallas_call(
        functools.partial(pack_kernel, pitch),
        out_shape=jax.ShapeDtypeStruct((LANES, used, LANES), BF),
        in_specs=[pl.BlockSpec(memory_space=pltpu.VMEM)],
        out_specs=pl.BlockSpec(memory_space=pltpu.VMEM),
        scratch_shapes=[pltpu.VMEM((LANES * pitch, LANES), F32)],
        compiler_params=pltpu.CompilerParams(vmem_limit_bytes=VMEM_LIMIT),
    )(x)


def mid_kernel(
    acts, rows, pairs, items, r_ref, f_ref, m_ref, h_ref, out_ref, flat, unsel, padded, u_ref, w_ref, s_ref
):
    count = r_ref.shape[0] // acts
    wide = count * rows
    chunks = pairs * items // USED
    used = chunks * rows
    for k in range(chunks):
        for i in range(items):
            unsel[k * LANES : (k + 1) * LANES, i * LANES : (i + 1) * LANES] = onehot(
                (LANES, LANES), k * USED, i * pairs, USED, pairs
            )
    for j in range(acts):
        padded[j * LANES : (j + 1) * LANES, :] = onehot((LANES, acts * pairs), j * pairs, 0, pairs, acts * pairs)

    def spread(matrix):
        half = lax.dot_general(padded[...], matrix, NT_DIMS, preferred_element_type=F32).astype(BF)
        return lax.dot_general(half, padded[...], NT_DIMS, preferred_element_type=F32).astype(BF)

    m_wide = spread(m_ref[...])
    h_wide = spread(h_ref[...])

    def arrive(j, carry):
        for v in range(count):
            block = r_ref[j * count + v].astype(F32)
            for k in range(chunks):
                flat[v * rows : (v + 1) * rows, k * LANES : (k + 1) * LANES] = block[k * rows : (k + 1) * rows]
        u_ref[j] = jnp.dot(flat[...].astype(BF), unsel[...], preferred_element_type=F32).astype(BF)
        return carry

    lax.fori_loop(0, acts, arrive, 0)
    for i in range(items):
        cols = slice(i * LANES, (i + 1) * LANES)
        u = jnp.concatenate([u_ref[j, :, cols] for j in range(acts)], axis=1)
        w = jnp.dot(u, m_wide, preferred_element_type=F32).astype(BF)
        s = jnp.dot(f_ref[...], w, preferred_element_type=F32)
        s = (s + jnp.dot(u, h_wide, preferred_element_type=F32)).astype(BF)
        for j in range(acts):
            w_ref[j, :, cols] = w[:, j * LANES : (j + 1) * LANES]
            s_ref[j, :, cols] = s[:, j * LANES : (j + 1) * LANES]

    def leave(j, carry):
        for n, source in enumerate((w_ref, s_ref)):
            flat[...] = lax.dot_general(source[j], unsel[...], NT_DIMS, preferred_element_type=F32)
            for v in range(count):
                block = jnp.concatenate(
                    [
                        flat[v * rows : (v + 1) * rows, k * LANES : (k + 1) * LANES]
                        for k in range(chunks)
                    ],
                    axis=0,
                )
                out_ref[j * count + v, n * used : (n + 1) * used, :] = block.astype(BF)
        return carry

    lax.fori_loop(0, acts, leave, 0)


def middle(received, fock, metric, active, acts, rows, pairs, items):
    count = received.shape[0] // acts
    wide = count * rows
    chunks = pairs * items // USED
    vmem = pl.BlockSpec(memory_space=pltpu.VMEM)
    return pl.pallas_call(
        functools.partial(mid_kernel, acts, rows, pairs, items),
        out_shape=jax.ShapeDtypeStruct((LANES, 2 * chunks * rows, LANES), BF),
        in_specs=[vmem] * 4,
        out_specs=vmem,
        scratch_shapes=[
            pltpu.VMEM((wide, chunks * LANES), F32),
            pltpu.VMEM((chunks * LANES, items * LANES), BF),
            pltpu.VMEM((acts * LANES, acts * pairs), BF),
            pltpu.VMEM((acts, wide, items * LANES), BF),
            pltpu.VMEM((acts, wide, items * LANES), BF),
            pltpu.VMEM((acts, wide, items * LANES), BF),
        ],
        compiler_params=pltpu.CompilerParams(vmem_limit_bytes=VMEM_LIMIT),
    )(received, fock, metric, active)


def last_kernel(pitch, r_ref, x_ref, f_ref, sigma_ref, w_ref, sums_ref, scratch, w_all, s_all):
    rows, pairs, width = x_ref.shape
    items = width // LANES
    chunks = pairs * items // USED
    used = chunks * rows
    table = touching(pairs, items)
    tall = w_all.shape[0] // rows
    for d in range(LANES):
        scratch[d * pitch : d * pitch + 2 * used, :] = r_ref[d].astype(F32)
    sel = {
        (k, i): onehot((tall, LANES), i * pairs, k * USED, pairs, USED)
        for k in range(chunks)
        for i in table[k]
    }
    for a in range(rows):
        for n, target in enumerate((w_all, s_all)):
            got = [
                scratch[pl.ds(n * used + k * rows + a, LANES, stride=pitch), :].astype(BF)
                for k in range(chunks)
            ]
            for i in range(items):
                total = None
                for k in range(chunks):
                    if i in table[k]:
                        part = lax.dot_general(sel[k, i], got[k], NT_DIMS, preferred_element_type=F32)
                        total = part if total is None else total + part
                target[a * tall : (a + 1) * tall, i * LANES : (i + 1) * LANES] = total.astype(target.dtype)
    s_all[...] = s_all[...] + jnp.dot(w_all[...], f_ref[...], preferred_element_type=F32)
    sums = [jnp.zeros((1, width), F32)] * 5
    for a in range(rows):
        x = x_ref[a].astype(F32)
        w = w_all[a * tall : (a + 1) * tall, :]
        w_ref[a] = w[:pairs]
        w = w.astype(F32)[:pairs]
        s = s_all[a * tall : a * tall + pairs, :]
        sigma_ref[a] = s
        for n, product in enumerate((x * s, x * w, s * s, s * w, w * w)):
            sums[n] = sums[n] + jnp.sum(product, axis=0, keepdims=True)
    lane = lax.broadcasted_iota(jnp.int32, (1, LANES), 1)
    packed = jnp.zeros((1, LANES), F32)
    for n in range(5):
        packed = packed + jnp.where(lane == n, jnp.sum(sums[n]), 0.0)
    sums_ref[...] = packed


def last(received, x, fock):
    rows, pairs, width = x.shape
    used = received.shape[1] // 2
    tall = (pairs + 7) // 8 * 8
    pitch = 2 * used + 8
    vmem = pl.BlockSpec(memory_space=pltpu.VMEM)
    return pl.pallas_call(
        functools.partial(last_kernel, pitch),
        out_shape=(
            jax.ShapeDtypeStruct((rows, pairs, width), F32),
            jax.ShapeDtypeStruct((rows, pairs, width), BF),
            jax.ShapeDtypeStruct((1, LANES), F32),
        ),
        in_specs=[vmem] * 3,
        out_specs=(vmem, vmem, vmem),
        scratch_shapes=[
            pltpu.VMEM((LANES * pitch, LANES), F32),
            pltpu.VMEM((rows * tall, width), BF),
            pltpu.VMEM((rows * tall, width), F32),
        ],
        compiler_params=pltpu.CompilerParams(vmem_limit_bytes=VMEM_LIMIT),
    )(received, x, fock)


def exchange(value):
    return lax.all_to_all(value, ALL, split_axis=0, concat_axis=0, tiled=True)


def local(amplitudes, virtual_fock_block, metric, active_block):
    acts = lax.axis_size("act")
    x = jnp.transpose(amplitudes, (1, 0, 2))
    rows, pairs, width = x.shape
    items = width // LANES
    arrived = exchange(pack(x))
    sent = middle(arrived, virtual_fock_block, metric, active_block, acts, rows, pairs, items)
    sigma, weighted, partial = last(exchange(sent), x, virtual_fock_block)
    spread = jnp.broadcast_to(partial[None], (LANES,) + partial.shape)
    totals = jnp.sum(exchange(spread), axis=(0, 1))
    denominator = totals[1]
    rayleigh = totals[0] / denominator
    resid = sigma - rayleigh * weighted.astype(F32)
    squares = totals[2] - 2.0 * rayleigh * totals[3] + rayleigh * rayleigh * totals[4]
    return jnp.transpose(resid.astype(BF), (1, 0, 2)), rayleigh, squares / denominator


def solution(mesh):
    in_specs = (P("act", "virt", None), P(), P(), P())
    out_specs = (P("act", "virt", None), P(), P())
    return jax.shard_map(local, mesh=mesh, in_specs=in_specs, out_specs=out_specs, check_vma=False)
```

```python
import functools

import jax
import jax.numpy as jnp
from jax import lax
from jax.experimental import pallas as pl
from jax.experimental.pallas import tpu as pltpu
from jax.sharding import PartitionSpec as P

BF = jnp.bfloat16
F32 = jnp.float32
ALL = ("act", "virt")
LANES = 128
USED = 125
MIB = 1024 * 1024
PACK_LIMIT, MID_LIMIT, LAST_LIMIT, FINISH_LIMIT = 16 * MIB, 40 * MIB, 44 * MIB, 16 * MIB
NT_DIMS = (((1,), (1,)), ((), ()))
TN_DIMS = (((0,), (0,)), ((), ()))


def onehot(shape, row_base, column_base, row_end, column_end):
    rows = lax.broadcasted_iota(jnp.int32, shape, 0)
    columns = lax.broadcasted_iota(jnp.int32, shape, 1)
    same = (rows + row_base) == (columns + column_base)
    keep = same & (rows < row_end) & (columns < column_end)
    return jnp.where(keep, 1.0, 0.0).astype(BF)


def touching(pairs, items):
    chunks = pairs * items // USED
    return [
        [i for i in range(items) if i * pairs < (k + 1) * USED and (i + 1) * pairs > k * USED]
        for k in range(chunks)
    ]


def pack_kernel(pitch, x_ref, out_ref, scratch):
    rows, pairs, width = x_ref.shape
    items = width // LANES
    table = touching(pairs, items)
    chunks = len(table)
    sel = {
        (k, i): onehot((pairs, LANES), i * pairs, k * USED, pairs, USED)
        for k in range(chunks)
        for i in table[k]
    }
    for a in range(rows):
        for k in range(chunks):
            total = None
            for i in table[k]:
                part = lax.dot_general(
                    x_ref[a, :, i * LANES : (i + 1) * LANES], sel[k, i], TN_DIMS, preferred_element_type=F32
                )
                total = part if total is None else total + part
            scratch[pl.ds(k * rows + a, LANES, stride=pitch), :] = total
    used = chunks * rows
    for d in range(LANES):
        out_ref[d] = scratch[d * pitch : d * pitch + used, :].astype(BF)


def pack(x):
    rows, pairs, width = x.shape
    used = pairs * (width // LANES) // USED * rows
    pitch = used + 8
    return pl.pallas_call(
        functools.partial(pack_kernel, pitch),
        out_shape=jax.ShapeDtypeStruct((LANES, used, LANES), BF),
        in_specs=[pl.BlockSpec(memory_space=pltpu.VMEM)],
        out_specs=pl.BlockSpec(memory_space=pltpu.VMEM),
        scratch_shapes=[pltpu.VMEM((LANES * pitch, LANES), F32)],
        compiler_params=pltpu.CompilerParams(vmem_limit_bytes=PACK_LIMIT),
    )(x)


def pieces(item, pairs):
    first, end = item * pairs, (item + 1) * pairs
    return [
        (k, max(first, k * USED) - first, min(end, (k + 1) * USED) - first)
        for k in range(first // USED, (end - 1) // USED + 1)
    ]


def parts(chunk, pairs):
    first, end = chunk * USED, (chunk + 1) * USED
    return [
        (i, max(first, i * pairs) - first, min(end, (i + 1) * pairs) - first)
        for i in range(first // pairs, (end - 1) // pairs + 1)
    ]


def turned(tile, shift):
    shift %= LANES
    return tile if shift == 0 else pltpu.roll(tile, shift, 1)


def joined(found, lane):
    tile = found[0][0]
    for other, first in found[1:]:
        tile = jnp.where(lane >= first, other, tile)
    return tile


def mid_kernel(acts, rows, pairs, items, r_ref, f_ref, m_ref, h_ref, out_ref, flat, padded, u_ref, y_ref):
    count = r_ref.shape[0] // acts
    wide = count * rows
    chunks = pairs * items // USED
    used = chunks * rows
    span = acts * LANES
    lane = lax.broadcasted_iota(jnp.int32, (wide, LANES), 1)
    for j in range(acts):
        padded[j * LANES : (j + 1) * LANES, :] = onehot((LANES, acts * pairs), j * pairs, 0, pairs, acts * pairs)

    def spread(matrix):
        half = lax.dot_general(padded[...], matrix, NT_DIMS, preferred_element_type=F32).astype(BF)
        return lax.dot_general(half, padded[...], NT_DIMS, preferred_element_type=F32).astype(BF)

    m_wide = spread(m_ref[...])
    h_wide = spread(h_ref[...])
    for j in range(acts):
        for v in range(count):
            block = r_ref[j * count + v].astype(F32)
            for k in range(chunks):
                flat[v * rows : (v + 1) * rows, k * LANES : (k + 1) * LANES] = block[k * rows : (k + 1) * rows]
        for i in range(items):
            found = [
                (turned(flat[:, k * LANES : (k + 1) * LANES], k * USED - i * pairs), first)
                for k, first, end in pieces(i, pairs)
            ]
            u_ref[i, :, j * LANES : (j + 1) * LANES] = joined(found, lane).astype(BF)
    for i in range(items):
        w = jnp.dot(u_ref[i], m_wide, preferred_element_type=F32)
        y_ref[0, i] = w
        s = jnp.dot(f_ref[...], w.astype(BF), preferred_element_type=F32)
        y_ref[1, i] = s + jnp.dot(u_ref[i], h_wide, preferred_element_type=F32)
    for j in range(acts):
        for n in range(2):
            for k in range(chunks):
                found = [
                    (turned(y_ref[n, i, :, j * LANES : (j + 1) * LANES], i * pairs - k * USED), first)
                    for i, first, end in parts(k, pairs)
                ]
                flat[:, k * LANES : (k + 1) * LANES] = joined(found, lane)
            for v in range(count):
                block = jnp.concatenate(
                    [flat[v * rows : (v + 1) * rows, k * LANES : (k + 1) * LANES] for k in range(chunks)],
                    axis=0,
                )
                out_ref[j * count + v, n * used : (n + 1) * used, :] = block.astype(BF)


def middle(received, fock, metric, active, acts, rows, pairs, items):
    count = received.shape[0] // acts
    wide = count * rows
    chunks = pairs * items // USED
    vmem = pl.BlockSpec(memory_space=pltpu.VMEM)
    return pl.pallas_call(
        functools.partial(mid_kernel, acts, rows, pairs, items),
        out_shape=jax.ShapeDtypeStruct((LANES, 2 * chunks * rows, LANES), BF),
        in_specs=[vmem] * 4,
        out_specs=vmem,
        scratch_shapes=[
            pltpu.VMEM((wide, chunks * LANES), F32),
            pltpu.VMEM((acts * LANES, acts * pairs), BF),
            pltpu.VMEM((items, wide, acts * LANES), BF),
            pltpu.VMEM((2, items, wide, acts * LANES), F32),
        ],
        compiler_params=pltpu.CompilerParams(vmem_limit_bytes=MID_LIMIT),
    )(received, fock, metric, active)


def last_kernel(pitch, r_ref, x_ref, f_ref, sigma_ref, w_ref, sums_ref, scratch, w_all, s_all):
    rows, pairs, width = x_ref.shape
    items = width // LANES
    chunks = pairs * items // USED
    used = chunks * rows
    tall = w_all.shape[0] // rows
    for d in range(LANES):
        scratch[d * pitch : d * pitch + 2 * used, :] = r_ref[d].astype(F32)
    sel = [
        jnp.concatenate(
            [onehot((tall, LANES), i * pairs, k * USED, pairs, USED) for k, first, end in pieces(i, pairs)],
            axis=1,
        )
        for i in range(items)
    ]
    for a in range(0, rows, 2):
        for n, target in enumerate((w_all, s_all)):
            got = [
                jnp.concatenate(
                    [scratch[pl.ds(n * used + k * rows + b, LANES, stride=pitch), :] for b in (a, a + 1)],
                    axis=0,
                ).astype(BF)
                for k in range(chunks)
            ]
            for i in range(items):
                source = jnp.concatenate([got[k] for k, first, end in pieces(i, pairs)], axis=1)
                both = lax.dot_general(sel[i], source, NT_DIMS, preferred_element_type=F32)
                both = both.astype(target.dtype)
                for b in range(2):
                    target[(a + b) * tall : (a + b + 1) * tall, i * LANES : (i + 1) * LANES] = both[
                        :, b * LANES : (b + 1) * LANES
                    ]
    s_all[...] = s_all[...] + jnp.dot(w_all[...], f_ref[...], preferred_element_type=F32)
    sums = [jnp.zeros((1, width), F32)] * 5
    for a in range(rows):
        x = x_ref[a].astype(F32)
        w = w_all[a * tall : (a + 1) * tall, :]
        w_ref[a] = w[:pairs]
        w = w.astype(F32)[:pairs]
        s = s_all[a * tall : a * tall + pairs, :]
        sigma_ref[a] = s
        for n, product in enumerate((x * s, x * w, s * s, s * w, w * w)):
            sums[n] = sums[n] + jnp.sum(product, axis=0, keepdims=True)
    lane = lax.broadcasted_iota(jnp.int32, (1, LANES), 1)
    packed = jnp.zeros((1, LANES), F32)
    for n in range(5):
        packed = packed + jnp.where(lane == n, jnp.sum(sums[n]), 0.0)
    for d in range(sums_ref.shape[0]):
        sums_ref[d] = packed


def last(received, x, fock):
    rows, pairs, width = x.shape
    used = received.shape[1] // 2
    tall = (pairs + 7) // 8 * 8
    pitch = 2 * used + 8
    vmem = pl.BlockSpec(memory_space=pltpu.VMEM)
    return pl.pallas_call(
        functools.partial(last_kernel, pitch),
        out_shape=(
            jax.ShapeDtypeStruct((rows, pairs, width), F32),
            jax.ShapeDtypeStruct((rows, pairs, width), BF),
            jax.ShapeDtypeStruct((LANES, 1, LANES), F32),
        ),
        in_specs=[vmem] * 3,
        out_specs=(vmem, vmem, vmem),
        scratch_shapes=[
            pltpu.VMEM((LANES * pitch, LANES), F32),
            pltpu.VMEM((rows * tall, width), BF),
            pltpu.VMEM((rows * tall, width), F32),
        ],
        compiler_params=pltpu.CompilerParams(vmem_limit_bytes=LAST_LIMIT),
    )(received, x, fock)


def finish_kernel(sums_ref, sigma_ref, w_ref, resid_ref, ratio_ref, norm_ref):
    totals = jnp.sum(sums_ref[...], axis=0)
    lane = lax.broadcasted_iota(jnp.int32, totals.shape, 1)
    total = [jnp.sum(jnp.where(lane == n, totals, 0.0)) for n in range(5)]
    rayleigh = jnp.full((1, LANES), total[0]) / jnp.full((1, LANES), total[1])
    squares = total[2] - 2.0 * rayleigh * total[3] + rayleigh * rayleigh * total[4]
    ratio_ref[...] = rayleigh
    norm_ref[...] = squares / jnp.full((1, LANES), total[1])
    width = sigma_ref.shape[2]
    wide = jnp.concatenate([rayleigh] * (width // LANES), axis=1)
    for a in range(sigma_ref.shape[0]):
        resid_ref[a] = (sigma_ref[a] - wide * w_ref[a].astype(F32)).astype(BF)


def finish(sums, sigma, weighted):
    vmem = pl.BlockSpec(memory_space=pltpu.VMEM)
    row = jax.ShapeDtypeStruct((1, LANES), F32)
    return pl.pallas_call(
        finish_kernel,
        out_shape=(jax.ShapeDtypeStruct(weighted.shape, BF), row, row),
        in_specs=[vmem] * 3,
        out_specs=(vmem,) * 3,
        compiler_params=pltpu.CompilerParams(vmem_limit_bytes=FINISH_LIMIT),
    )(sums, sigma, weighted)


def exchange(value):
    return lax.all_to_all(value, ALL, split_axis=0, concat_axis=0, tiled=True)


def local(amplitudes, virtual_fock_block, metric, active_block):
    acts = lax.axis_size("act")
    x = jnp.transpose(amplitudes, (1, 0, 2))
    rows, pairs, width = x.shape
    items = width // LANES
    arrived = exchange(pack(x))
    sent = middle(arrived, virtual_fock_block, metric, active_block, acts, rows, pairs, items)
    sigma, weighted, partial = last(exchange(sent), x, virtual_fock_block)
    resid, rayleigh, norm = finish(exchange(partial), sigma, weighted)
    return jnp.transpose(resid, (1, 0, 2)), rayleigh[0, 0], norm[0, 0]


def solution(mesh):
    in_specs = (P("act", "virt", None), P(), P(), P())
    out_specs = (P("act", "virt", None), P(), P())
    return jax.shard_map(local, mesh=mesh, in_specs=in_specs, out_specs=out_specs, check_vma=False)
```

```python
import functools

import jax
import jax.numpy as jnp
from jax import lax
from jax.experimental import pallas as pl
from jax.experimental.pallas import tpu as pltpu
from jax.sharding import PartitionSpec as P

BF = jnp.bfloat16
F32 = jnp.float32
ALL = ("act", "virt")
LANES = 128
USED = 125
MIB = 1024 * 1024
PACK_LIMIT, MID_LIMIT, LAST_LIMIT, FINISH_LIMIT = 16 * MIB, 26 * MIB, 32 * MIB, 8 * MIB
LANES_ROWS = 104
NT_DIMS = (((1,), (1,)), ((), ()))
TN_DIMS = (((0,), (0,)), ((), ()))


def onehot(shape, row_base, column_base, row_end, column_end):
    rows = lax.broadcasted_iota(jnp.int32, shape, 0)
    columns = lax.broadcasted_iota(jnp.int32, shape, 1)
    same = (rows + row_base) == (columns + column_base)
    keep = same & (rows < row_end) & (columns < column_end)
    return jnp.where(keep, 1.0, 0.0).astype(BF)


def touching(pairs, items):
    chunks = pairs * items // USED
    return [
        [i for i in range(items) if i * pairs < (k + 1) * USED and (i + 1) * pairs > k * USED]
        for k in range(chunks)
    ]


def pack_kernel(acts, pitch, x_hbm, m_hbm, h_hbm, out_ref, wide_ref, x_ref, m_ref, h_ref, scratch, padded, sems):
    rows, pairs, width = x_hbm.shape
    items = width // LANES
    table = touching(pairs, items)
    chunks = len(table)
    pairs_of = ((m_hbm, m_ref), (h_hbm, h_ref), (x_hbm, x_ref))
    copies = [pltpu.make_async_copy(a, b, sems.at[n]) for n, (a, b) in enumerate(pairs_of)]
    for copy in copies:
        copy.start()
    span = acts * LANES
    for j in range(acts):
        padded[j * LANES : (j + 1) * LANES, :] = onehot((LANES, acts * pairs), j * pairs, 0, pairs, acts * pairs)
    for n, matrix in enumerate((m_ref, h_ref)):
        copies[n].wait()
        half = lax.dot_general(padded[...], matrix[...], NT_DIMS, preferred_element_type=F32).astype(BF)
        wide = lax.dot_general(half, padded[...], NT_DIMS, preferred_element_type=F32)
        wide_ref[:, n * span : (n + 1) * span] = wide.astype(BF)
    sel = {
        (k, i): onehot((pairs, LANES), i * pairs, k * USED, pairs, USED)
        for k in range(chunks)
        for i in table[k]
    }
    copies[2].wait()
    for a in range(rows):
        for k in range(chunks):
            total = None
            for i in table[k]:
                part = lax.dot_general(
                    x_ref[a, :, i * LANES : (i + 1) * LANES], sel[k, i], TN_DIMS, preferred_element_type=F32
                )
                total = part if total is None else total + part
            scratch[pl.ds(k * rows + a, LANES, stride=pitch), :] = total
    used = chunks * rows
    for d in range(LANES):
        out_ref[d] = scratch[d * pitch : d * pitch + used, :].astype(BF)


def pack(x, metric, active, acts):
    rows, pairs, width = x.shape
    used = pairs * (width // LANES) // USED * rows
    pitch = used + 8
    span = acts * LANES
    vmem = pl.BlockSpec(memory_space=pltpu.VMEM)
    return pl.pallas_call(
        functools.partial(pack_kernel, acts, pitch),
        out_shape=(
            jax.ShapeDtypeStruct((LANES, used, LANES), BF),
            jax.ShapeDtypeStruct((span, 2 * span), BF),
        ),
        in_specs=[pl.BlockSpec(memory_space=pltpu.HBM)] * 3,
        out_specs=(vmem, vmem),
        scratch_shapes=[
            pltpu.VMEM(x.shape, BF),
            pltpu.VMEM(metric.shape, BF),
            pltpu.VMEM(active.shape, BF),
            pltpu.VMEM((LANES * pitch, LANES), F32),
            pltpu.VMEM((span, acts * pairs), BF),
            pltpu.SemaphoreType.DMA((3,)),
        ],
        compiler_params=pltpu.CompilerParams(vmem_limit_bytes=PACK_LIMIT),
    )(*(pltpu.with_memory_space_constraint(a, pltpu.HBM) for a in (x, metric, active)))


def pieces(item, pairs):
    first, end = item * pairs, (item + 1) * pairs
    return [
        (k, max(first, k * USED) - first, min(end, (k + 1) * USED) - first)
        for k in range(first // USED, (end - 1) // USED + 1)
    ]


def parts(chunk, pairs):
    first, end = chunk * USED, (chunk + 1) * USED
    return [
        (i, max(first, i * pairs) - first, min(end, (i + 1) * pairs) - first)
        for i in range(first // pairs, (end - 1) // pairs + 1)
    ]


def turned(tile, shift):
    shift %= LANES
    return tile if shift == 0 else pltpu.roll(tile, shift, 1)


def joined(found, lane):
    tile = found[0][0]
    for other, first in found[1:]:
        tile = jnp.where(lane >= first, other, tile)
    return tile


def mid_kernel(acts, rows, pairs, items, r_ref, f_ref, wide_ref, out_ref, flat, u_ref, y_ref):
    count = r_ref.shape[0] // acts
    tall = count * rows
    chunks = pairs * items // USED
    used = chunks * rows
    lane = lax.broadcasted_iota(jnp.int32, (tall, LANES), 1)
    for j in range(acts):
        for v in range(count):
            block = r_ref[j * count + v].astype(F32)
            for k in range(chunks):
                flat[0, v * rows : (v + 1) * rows, k * LANES : (k + 1) * LANES] = block[k * rows : (k + 1) * rows]
        for i in range(items):
            found = [
                (turned(flat[0, :, k * LANES : (k + 1) * LANES], k * USED - i * pairs), first)
                for k, first, end in pieces(i, pairs)
            ]
            u_ref[i, :, j * LANES : (j + 1) * LANES] = joined(found, lane).astype(BF)
    for i in range(items):
        y_ref[i] = jnp.dot(u_ref[i], wide_ref[...], preferred_element_type=F32)
    for j in range(acts):
        for n in range(2):
            at = (n * acts + j) * LANES
            for k in range(chunks):
                found = [
                    (turned(y_ref[i, :, at : at + LANES], i * pairs - k * USED), first)
                    for i, first, end in parts(k, pairs)
                ]
                flat[n, :, k * LANES : (k + 1) * LANES] = joined(found, lane)
        flat[1] = flat[1] + jnp.dot(f_ref[...], flat[0].astype(BF), preferred_element_type=F32)
        for n in range(2):
            for v in range(count):
                block = jnp.concatenate(
                    [flat[n, v * rows : (v + 1) * rows, k * LANES : (k + 1) * LANES] for k in range(chunks)],
                    axis=0,
                )
                out_ref[j * count + v, n * used : (n + 1) * used, :] = block.astype(BF)


def middle(received, fock, wide, acts, rows, pairs, items):
    count = received.shape[0] // acts
    tall = count * rows
    chunks = pairs * items // USED
    vmem = pl.BlockSpec(memory_space=pltpu.VMEM)
    return pl.pallas_call(
        functools.partial(mid_kernel, acts, rows, pairs, items),
        out_shape=jax.ShapeDtypeStruct((LANES, 2 * chunks * rows, LANES), BF),
        in_specs=[vmem] * 3,
        out_specs=vmem,
        scratch_shapes=[
            pltpu.VMEM((2, tall, chunks * LANES), F32),
            pltpu.VMEM((items, tall, acts * LANES), BF),
            pltpu.VMEM((items, tall, 2 * acts * LANES), F32),
        ],
        compiler_params=pltpu.CompilerParams(vmem_limit_bytes=MID_LIMIT),
    )(received, fock, wide)


def last_kernel(pitch, r_ref, x_ref, f_ref, sigma_ref, w_ref, sums_ref, scratch, w_all, s_all):
    rows, pairs, width = x_ref.shape
    items = width // LANES
    chunks = pairs * items // USED
    used = chunks * rows
    group, tall = w_all.shape[0] // LANES_ROWS, LANES_ROWS
    whole = pairs // 8 * 8
    for d in range(LANES):
        scratch[d * pitch : d * pitch + 2 * used, :] = r_ref[d].astype(F32)
    sel = [
        jnp.concatenate(
            [onehot((tall, LANES), i * pairs, k * USED, pairs, USED) for k, first, end in pieces(i, pairs)],
            axis=1,
        )
        for i in range(items)
    ]
    sums = [jnp.zeros((8, width), F32)] * 5
    for base in range(0, rows, group):
        for a in range(0, group, 2):
            for n, target in enumerate((w_all, s_all)):
                got = [
                    jnp.concatenate(
                        [
                            scratch[pl.ds(n * used + k * rows + base + b, LANES, stride=pitch), :]
                            for b in (a, a + 1)
                        ],
                        axis=0,
                    ).astype(BF)
                    for k in range(chunks)
                ]
                for i in range(items):
                    source = jnp.concatenate([got[k] for k, first, end in pieces(i, pairs)], axis=1)
                    both = lax.dot_general(sel[i], source, NT_DIMS, preferred_element_type=F32)
                    both = both.astype(target.dtype)
                    for b in range(2):
                        target[(a + b) * tall : (a + b + 1) * tall, i * LANES : (i + 1) * LANES] = both[
                            :, b * LANES : (b + 1) * LANES
                        ]
        s_all[...] = s_all[...] + jnp.dot(w_all[...], f_ref[...], preferred_element_type=F32)
        for a in range(group):
            w_ref[base + a] = w_all[a * tall : a * tall + pairs, :]
            sigma_ref[base + a] = s_all[a * tall : a * tall + pairs, :]
            for first, end in ((0, whole), (whole, pairs)):
                x = x_ref[base + a, first:end].astype(F32)
                w = w_all[a * tall + first : a * tall + end, :].astype(F32)
                s = s_all[a * tall + first : a * tall + end, :]
                for n, product in enumerate((x * s, x * w, s * s, s * w, w * w)):
                    if end - first >= 8:
                        product = jnp.sum(product.reshape(-1, 8, width), axis=0)
                    else:
                        product = jnp.concatenate(
                            [product, jnp.zeros((8 - (end - first), width), F32)], axis=0
                        )
                    sums[n] = sums[n] + product
    lane = lax.broadcasted_iota(jnp.int32, (1, LANES), 1)
    packed = jnp.zeros((1, LANES), F32)
    for n in range(5):
        packed = packed + jnp.where(lane == n, jnp.sum(sums[n]), 0.0)
    for d in range(sums_ref.shape[0]):
        sums_ref[d] = packed


def last(received, x, fock):
    rows, pairs, width = x.shape
    used = received.shape[1] // 2
    pitch = 2 * used + 8
    group = rows
    vmem = pl.BlockSpec(memory_space=pltpu.VMEM)
    return pl.pallas_call(
        functools.partial(last_kernel, pitch),
        out_shape=(
            jax.ShapeDtypeStruct((rows, pairs, width), F32),
            jax.ShapeDtypeStruct((rows, pairs, width), BF),
            jax.ShapeDtypeStruct((LANES, 1, LANES), F32),
        ),
        in_specs=[vmem] * 3,
        out_specs=(vmem, vmem, vmem),
        scratch_shapes=[
            pltpu.VMEM((LANES * pitch, LANES), F32),
            pltpu.VMEM((group * LANES_ROWS, width), BF),
            pltpu.VMEM((group * LANES_ROWS, width), F32),
        ],
        compiler_params=pltpu.CompilerParams(vmem_limit_bytes=LAST_LIMIT),
    )(received, x, fock)


def finish_kernel(sums_ref, sigma_ref, w_ref, resid_hbm, ratio_ref, norm_ref, resid_ref, sems):
    totals = jnp.sum(sums_ref[...], axis=0)
    lane = lax.broadcasted_iota(jnp.int32, totals.shape, 1)
    total = [jnp.sum(jnp.where(lane == n, totals, 0.0)) for n in range(5)]
    rayleigh = jnp.full((1, LANES), total[0]) / jnp.full((1, LANES), total[1])
    squares = total[2] - 2.0 * rayleigh * total[3] + rayleigh * rayleigh * total[4]
    ratio_ref[...] = rayleigh
    norm_ref[...] = squares / jnp.full((1, LANES), total[1])
    rows, pairs, width = sigma_ref.shape
    wide = jnp.concatenate([rayleigh] * (width // LANES), axis=1)
    group = rows // sems.shape[0]
    copies = []
    for a in range(rows):
        resid_ref[a] = (sigma_ref[a] - wide * w_ref[a].astype(F32)).astype(BF)
        if (a + 1) % group == 0:
            part = pl.ds(a + 1 - group, group)
            copies.append(pltpu.make_async_copy(resid_ref.at[part], resid_hbm.at[part], sems.at[a // group]))
            copies[-1].start()
    for copy in copies:
        copy.wait()


def finish(sums, sigma, weighted):
    vmem = pl.BlockSpec(memory_space=pltpu.VMEM)
    row = jax.ShapeDtypeStruct((1, LANES), F32)
    return pl.pallas_call(
        finish_kernel,
        out_shape=(jax.ShapeDtypeStruct(weighted.shape, BF), row, row),
        in_specs=[vmem] * 3,
        out_specs=(pl.BlockSpec(memory_space=pltpu.HBM), vmem, vmem),
        scratch_shapes=[pltpu.VMEM(weighted.shape, BF), pltpu.SemaphoreType.DMA((5,))],
        compiler_params=pltpu.CompilerParams(vmem_limit_bytes=FINISH_LIMIT),
    )(sums, sigma, weighted)


def exchange(value):
    return lax.all_to_all(value, ALL, split_axis=0, concat_axis=0, tiled=True)


def local(amplitudes, virtual_fock_block, metric, active_block):
    acts = lax.axis_size("act")
    x = jnp.transpose(amplitudes, (1, 0, 2))
    rows, pairs, width = x.shape
    items = width // LANES
    packed, wide = pack(x, metric, active_block, acts)
    arrived = exchange(packed)
    sent = middle(arrived, virtual_fock_block, wide, acts, rows, pairs, items)
    sigma, weighted, partial = last(exchange(sent), x, virtual_fock_block)
    resid, rayleigh, norm = finish(exchange(partial), sigma, weighted)
    return jnp.transpose(resid, (1, 0, 2)), rayleigh[0, 0], norm[0, 0]


def solution(mesh):
    in_specs = (P("act", "virt", None), P(), P(), P())
    out_specs = (P("act", "virt", None), P(), P())
    return jax.shard_map(local, mesh=mesh, in_specs=in_specs, out_specs=out_specs, check_vma=False)
```

```python
import functools

import jax
import jax.numpy as jnp
from jax import lax
from jax.experimental import pallas as pl
from jax.experimental.pallas import tpu as pltpu
from jax.sharding import Mesh
from jax.sharding import PartitionSpec as P

BF = jnp.bfloat16
F32 = jnp.float32
VIRT = ("virt_0", "virt_1", "core")
ALL = ("core", "act", "virt_0", "virt_1")
LANES = 128
USED = 125
MIB = 1024 * 1024
PACK_LIMIT, MID_LIMIT, LAST_LIMIT, FINISH_LIMIT = 16 * MIB, 26 * MIB, 32 * MIB, 8 * MIB
LANES_ROWS = 104
NT_DIMS = (((1,), (1,)), ((), ()))
TN_DIMS = (((0,), (0,)), ((), ()))


def onehot(shape, row_base, column_base, row_end, column_end):
    rows = lax.broadcasted_iota(jnp.int32, shape, 0)
    columns = lax.broadcasted_iota(jnp.int32, shape, 1)
    same = (rows + row_base) == (columns + column_base)
    keep = same & (rows < row_end) & (columns < column_end)
    return jnp.where(keep, 1.0, 0.0).astype(BF)


def touching(pairs, items):
    chunks = pairs * items // USED
    return [
        [i for i in range(items) if i * pairs < (k + 1) * USED and (i + 1) * pairs > k * USED]
        for k in range(chunks)
    ]


def pack_kernel(acts, pitch, x_hbm, m_hbm, h_hbm, out_ref, wide_ref, x_ref, m_ref, h_ref, scratch, padded, sems):
    rows, pairs, width = x_hbm.shape
    items = width // LANES
    table = touching(pairs, items)
    chunks = len(table)
    pairs_of = ((m_hbm, m_ref), (h_hbm, h_ref), (x_hbm, x_ref))
    copies = [pltpu.make_async_copy(a, b, sems.at[n]) for n, (a, b) in enumerate(pairs_of)]
    for copy in copies:
        copy.start()
    span = acts * LANES
    for j in range(acts):
        padded[j * LANES : (j + 1) * LANES, :] = onehot((LANES, acts * pairs), j * pairs, 0, pairs, acts * pairs)
    for n, matrix in enumerate((m_ref, h_ref)):
        copies[n].wait()
        half = lax.dot_general(padded[...], matrix[...], NT_DIMS, preferred_element_type=F32).astype(BF)
        wide = lax.dot_general(half, padded[...], NT_DIMS, preferred_element_type=F32)
        wide_ref[:, n * span : (n + 1) * span] = wide.astype(BF)
    sel = {
        (k, i): onehot((pairs, LANES), i * pairs, k * USED, pairs, USED)
        for k in range(chunks)
        for i in table[k]
    }
    copies[2].wait()
    for a in range(rows):
        for k in range(chunks):
            total = None
            for i in table[k]:
                part = lax.dot_general(
                    x_ref[a, :, i * LANES : (i + 1) * LANES], sel[k, i], TN_DIMS, preferred_element_type=F32
                )
                total = part if total is None else total + part
            scratch[pl.ds(k * rows + a, LANES, stride=pitch), :] = total
    used = chunks * rows
    for d in range(LANES):
        out_ref[d] = scratch[d * pitch : d * pitch + used, :].astype(BF)


def pack(x, metric, active, acts):
    rows, pairs, width = x.shape
    used = pairs * (width // LANES) // USED * rows
    pitch = used + 8
    span = acts * LANES
    vmem = pl.BlockSpec(memory_space=pltpu.VMEM)
    return pl.pallas_call(
        functools.partial(pack_kernel, acts, pitch),
        out_shape=(
            jax.ShapeDtypeStruct((LANES, used, LANES), BF),
            jax.ShapeDtypeStruct((span, 2 * span), BF),
        ),
        in_specs=[pl.BlockSpec(memory_space=pltpu.HBM)] * 3,
        out_specs=(vmem, vmem),
        scratch_shapes=[
            pltpu.VMEM(x.shape, BF),
            pltpu.VMEM(metric.shape, BF),
            pltpu.VMEM(active.shape, BF),
            pltpu.VMEM((LANES * pitch, LANES), F32),
            pltpu.VMEM((span, acts * pairs), BF),
            pltpu.SemaphoreType.DMA((3,)),
        ],
        compiler_params=pltpu.CompilerParams(vmem_limit_bytes=PACK_LIMIT),
    )(*(pltpu.with_memory_space_constraint(a, pltpu.HBM) for a in (x, metric, active)))


def pieces(item, pairs):
    first, end = item * pairs, (item + 1) * pairs
    return [
        (k, max(first, k * USED) - first, min(end, (k + 1) * USED) - first)
        for k in range(first // USED, (end - 1) // USED + 1)
    ]


def parts(chunk, pairs):
    first, end = chunk * USED, (chunk + 1) * USED
    return [
        (i, max(first, i * pairs) - first, min(end, (i + 1) * pairs) - first)
        for i in range(first // pairs, (end - 1) // pairs + 1)
    ]


def turned(tile, shift):
    shift %= LANES
    return tile if shift == 0 else pltpu.roll(tile, shift, 1)


def joined(found, lane):
    tile = found[0][0]
    for other, first in found[1:]:
        tile = jnp.where(lane >= first, other, tile)
    return tile


def place(j, v, acts, count):
    return ((v % 2) * acts + j) * (count // 2) + v // 2


def mid_kernel(acts, rows, pairs, items, r_ref, f_ref, wide_ref, out_ref, flat, u_ref, y_ref):
    count = r_ref.shape[0] // acts
    tall = count * rows
    chunks = pairs * items // USED
    used = chunks * rows
    lane = lax.broadcasted_iota(jnp.int32, (tall, LANES), 1)
    for j in range(acts):
        for v in range(count):
            block = r_ref[place(j, v, acts, count)].astype(F32)
            for k in range(chunks):
                flat[0, v * rows : (v + 1) * rows, k * LANES : (k + 1) * LANES] = block[k * rows : (k + 1) * rows]
        for i in range(items):
            found = [
                (turned(flat[0, :, k * LANES : (k + 1) * LANES], k * USED - i * pairs), first)
                for k, first, end in pieces(i, pairs)
            ]
            u_ref[i, :, j * LANES : (j + 1) * LANES] = joined(found, lane).astype(BF)
    for i in range(items):
        y_ref[i] = jnp.dot(u_ref[i], wide_ref[...], preferred_element_type=F32)
    for j in range(acts):
        for n in range(2):
            at = (n * acts + j) * LANES
            for k in range(chunks):
                found = [
                    (turned(y_ref[i, :, at : at + LANES], i * pairs - k * USED), first)
                    for i, first, end in parts(k, pairs)
                ]
                flat[n, :, k * LANES : (k + 1) * LANES] = joined(found, lane)
        flat[1] = flat[1] + jnp.dot(f_ref[...], flat[0].astype(BF), preferred_element_type=F32)
        for n in range(2):
            for v in range(count):
                block = jnp.concatenate(
                    [flat[n, v * rows : (v + 1) * rows, k * LANES : (k + 1) * LANES] for k in range(chunks)],
                    axis=0,
                )
                out_ref[place(j, v, acts, count), n * used : (n + 1) * used, :] = block.astype(BF)


def middle(received, fock, wide, acts, rows, pairs, items):
    count = received.shape[0] // acts
    tall = count * rows
    chunks = pairs * items // USED
    vmem = pl.BlockSpec(memory_space=pltpu.VMEM)
    return pl.pallas_call(
        functools.partial(mid_kernel, acts, rows, pairs, items),
        out_shape=jax.ShapeDtypeStruct((LANES, 2 * chunks * rows, LANES), BF),
        in_specs=[vmem] * 3,
        out_specs=vmem,
        scratch_shapes=[
            pltpu.VMEM((2, tall, chunks * LANES), F32),
            pltpu.VMEM((items, tall, acts * LANES), BF),
            pltpu.VMEM((items, tall, 2 * acts * LANES), F32),
        ],
        compiler_params=pltpu.CompilerParams(vmem_limit_bytes=MID_LIMIT),
    )(received, fock, wide)


def last_kernel(pitch, r_ref, x_ref, f_ref, sigma_ref, w_ref, sums_ref, scratch, w_all, s_all):
    rows, pairs, width = x_ref.shape
    items = width // LANES
    chunks = pairs * items // USED
    used = chunks * rows
    group, tall = w_all.shape[0] // LANES_ROWS, LANES_ROWS
    whole = pairs // 8 * 8
    for d in range(LANES):
        scratch[d * pitch : d * pitch + 2 * used, :] = r_ref[d].astype(F32)
    sel = [
        jnp.concatenate(
            [onehot((tall, LANES), i * pairs, k * USED, pairs, USED) for k, first, end in pieces(i, pairs)],
            axis=1,
        )
        for i in range(items)
    ]
    sums = [jnp.zeros((8, width), F32)] * 5
    for base in range(0, rows, group):
        for a in range(0, group, 2):
            for n, target in enumerate((w_all, s_all)):
                got = [
                    jnp.concatenate(
                        [
                            scratch[pl.ds(n * used + k * rows + base + b, LANES, stride=pitch), :]
                            for b in (a, a + 1)
                        ],
                        axis=0,
                    ).astype(BF)
                    for k in range(chunks)
                ]
                for i in range(items):
                    source = jnp.concatenate([got[k] for k, first, end in pieces(i, pairs)], axis=1)
                    both = lax.dot_general(sel[i], source, NT_DIMS, preferred_element_type=F32)
                    both = both.astype(target.dtype)
                    for b in range(2):
                        target[(a + b) * tall : (a + b + 1) * tall, i * LANES : (i + 1) * LANES] = both[
                            :, b * LANES : (b + 1) * LANES
                        ]
        s_all[...] = s_all[...] + jnp.dot(w_all[...], f_ref[...], preferred_element_type=F32)
        for a in range(group):
            w_ref[base + a] = w_all[a * tall : a * tall + pairs, :]
            sigma_ref[base + a] = s_all[a * tall : a * tall + pairs, :]
            for first, end in ((0, whole), (whole, pairs)):
                x = x_ref[base + a, first:end].astype(F32)
                w = w_all[a * tall + first : a * tall + end, :].astype(F32)
                s = s_all[a * tall + first : a * tall + end, :]
                for n, product in enumerate((x * s, x * w, s * s, s * w, w * w)):
                    if end - first >= 8:
                        product = jnp.sum(product.reshape(-1, 8, width), axis=0)
                    else:
                        product = jnp.concatenate(
                            [product, jnp.zeros((8 - (end - first), width), F32)], axis=0
                        )
                    sums[n] = sums[n] + product
    lane = lax.broadcasted_iota(jnp.int32, (1, LANES), 1)
    packed = jnp.zeros((1, LANES), F32)
    for n in range(5):
        packed = packed + jnp.where(lane == n, jnp.sum(sums[n]), 0.0)
    for d in range(sums_ref.shape[0]):
        sums_ref[d] = packed


def last(received, x, fock):
    rows, pairs, width = x.shape
    used = received.shape[1] // 2
    pitch = 2 * used + 8
    group = rows
    vmem = pl.BlockSpec(memory_space=pltpu.VMEM)
    return pl.pallas_call(
        functools.partial(last_kernel, pitch),
        out_shape=(
            jax.ShapeDtypeStruct((rows, pairs, width), F32),
            jax.ShapeDtypeStruct((rows, pairs, width), BF),
            jax.ShapeDtypeStruct((LANES, 1, LANES), F32),
        ),
        in_specs=[vmem] * 3,
        out_specs=(vmem, vmem, vmem),
        scratch_shapes=[
            pltpu.VMEM((LANES * pitch, LANES), F32),
            pltpu.VMEM((group * LANES_ROWS, width), BF),
            pltpu.VMEM((group * LANES_ROWS, width), F32),
        ],
        compiler_params=pltpu.CompilerParams(vmem_limit_bytes=LAST_LIMIT),
    )(received, x, fock)


def finish_kernel(sums_ref, sigma_ref, w_ref, resid_hbm, ratio_ref, norm_ref, resid_ref, sems):
    totals = jnp.sum(sums_ref[...], axis=0)
    lane = lax.broadcasted_iota(jnp.int32, totals.shape, 1)
    total = [jnp.sum(jnp.where(lane == n, totals, 0.0)) for n in range(5)]
    rayleigh = jnp.full((1, LANES), total[0]) / jnp.full((1, LANES), total[1])
    squares = total[2] - 2.0 * rayleigh * total[3] + rayleigh * rayleigh * total[4]
    ratio_ref[...] = rayleigh
    norm_ref[...] = squares / jnp.full((1, LANES), total[1])
    rows, pairs, width = sigma_ref.shape
    wide = jnp.concatenate([rayleigh] * (width // LANES), axis=1)
    group = rows // sems.shape[0]
    copies = []
    for a in range(rows):
        resid_ref[a] = (sigma_ref[a] - wide * w_ref[a].astype(F32)).astype(BF)
        if (a + 1) % group == 0:
            part = pl.ds(a + 1 - group, group)
            copies.append(pltpu.make_async_copy(resid_ref.at[part], resid_hbm.at[part], sems.at[a // group]))
            copies[-1].start()
    for copy in copies:
        copy.wait()


def finish(sums, sigma, weighted):
    vmem = pl.BlockSpec(memory_space=pltpu.VMEM)
    row = jax.ShapeDtypeStruct((1, LANES), F32)
    return pl.pallas_call(
        finish_kernel,
        out_shape=(jax.ShapeDtypeStruct(weighted.shape, BF), row, row),
        in_specs=[vmem] * 3,
        out_specs=(pl.BlockSpec(memory_space=pltpu.HBM), vmem, vmem),
        scratch_shapes=[pltpu.VMEM(weighted.shape, BF), pltpu.SemaphoreType.DMA((5,))],
        compiler_params=pltpu.CompilerParams(vmem_limit_bytes=FINISH_LIMIT),
    )(sums, sigma, weighted)


def exchange(value):
    return lax.all_to_all(value, ALL, split_axis=0, concat_axis=0, tiled=True)


def local(amplitudes, virtual_fock_block, metric, active_block):
    acts = lax.axis_size("act")
    x = jnp.transpose(amplitudes, (1, 0, 2))
    rows, pairs, width = x.shape
    items = width // LANES
    packed, wide = pack(x, metric, active_block, acts)
    arrived = exchange(packed)
    sent = middle(arrived, virtual_fock_block, wide, acts, rows, pairs, items)
    sigma, weighted, partial = last(exchange(sent), x, virtual_fock_block)
    resid, rayleigh, norm = finish(exchange(partial), sigma, weighted)
    return jnp.transpose(resid, (1, 0, 2)), rayleigh[0, 0], norm[0, 0]


def solution(mesh):
    acts, virts = mesh.shape["act"], mesh.shape["virt"]
    torus = Mesh(mesh.devices.reshape(acts, 4, virts // 8, 2), ("act",) + VIRT)
    in_specs = (P("act", VIRT, None), P(), P(), P())
    out_specs = (P("act", VIRT, None), P(), P())
    return jax.shard_map(local, mesh=torus, in_specs=in_specs, out_specs=out_specs, check_vma=False)
```

```python
import functools

import jax
import jax.numpy as jnp
from jax import lax
from jax.experimental import pallas as pl
from jax.experimental.pallas import tpu as pltpu
from jax.sharding import Mesh
from jax.sharding import PartitionSpec as P

BF = jnp.bfloat16
F32 = jnp.float32
VIRT = ("virt_0", "virt_1", "core")
ALL = ("act", "core", "virt_0", "virt_1")
LANES = 128
USED = 125
MIB = 1024 * 1024
PACK_LIMIT, MID_LIMIT, LAST_LIMIT, FINISH_LIMIT = 16 * MIB, 26 * MIB, 32 * MIB, 8 * MIB
LANES_ROWS = 104
NT_DIMS = (((1,), (1,)), ((), ()))
TN_DIMS = (((0,), (0,)), ((), ()))


def onehot(shape, row_base, column_base, row_end, column_end):
    rows = lax.broadcasted_iota(jnp.int32, shape, 0)
    columns = lax.broadcasted_iota(jnp.int32, shape, 1)
    same = (rows + row_base) == (columns + column_base)
    keep = same & (rows < row_end) & (columns < column_end)
    return jnp.where(keep, 1.0, 0.0).astype(BF)


def touching(pairs, items):
    chunks = pairs * items // USED
    return [
        [i for i in range(items) if i * pairs < (k + 1) * USED and (i + 1) * pairs > k * USED]
        for k in range(chunks)
    ]


def pack_kernel(acts, pitch, x_hbm, m_hbm, h_hbm, out_ref, wide_ref, x_ref, m_ref, h_ref, scratch, padded, sems):
    rows, pairs, width = x_hbm.shape
    items = width // LANES
    table = touching(pairs, items)
    chunks = len(table)
    pairs_of = ((m_hbm, m_ref), (h_hbm, h_ref), (x_hbm, x_ref))
    copies = [pltpu.make_async_copy(a, b, sems.at[n]) for n, (a, b) in enumerate(pairs_of)]
    for copy in copies:
        copy.start()
    span = acts * LANES
    for j in range(acts):
        padded[j * LANES : (j + 1) * LANES, :] = onehot((LANES, acts * pairs), j * pairs, 0, pairs, acts * pairs)
    for n, matrix in enumerate((m_ref, h_ref)):
        copies[n].wait()
        half = lax.dot_general(padded[...], matrix[...], NT_DIMS, preferred_element_type=F32).astype(BF)
        wide = lax.dot_general(half, padded[...], NT_DIMS, preferred_element_type=F32)
        wide_ref[:, n * span : (n + 1) * span] = wide.astype(BF)
    sel = {
        (k, i): onehot((pairs, LANES), i * pairs, k * USED, pairs, USED)
        for k in range(chunks)
        for i in table[k]
    }
    copies[2].wait()
    for a in range(rows):
        for k in range(chunks):
            total = None
            for i in table[k]:
                part = lax.dot_general(
                    x_ref[a, :, i * LANES : (i + 1) * LANES], sel[k, i], TN_DIMS, preferred_element_type=F32
                )
                total = part if total is None else total + part
            scratch[pl.ds(k * rows + a, LANES, stride=pitch), :] = total
    used = chunks * rows
    for d in range(LANES):
        out_ref[d] = scratch[d * pitch : d * pitch + used, :].astype(BF)


def pack(x, metric, active, acts):
    rows, pairs, width = x.shape
    used = pairs * (width // LANES) // USED * rows
    pitch = used + 8
    span = acts * LANES
    vmem = pl.BlockSpec(memory_space=pltpu.VMEM)
    return pl.pallas_call(
        functools.partial(pack_kernel, acts, pitch),
        out_shape=(
            jax.ShapeDtypeStruct((LANES, used, LANES), BF),
            jax.ShapeDtypeStruct((span, 2 * span), BF),
        ),
        in_specs=[pl.BlockSpec(memory_space=pltpu.HBM)] * 3,
        out_specs=(vmem, vmem),
        scratch_shapes=[
            pltpu.VMEM(x.shape, BF),
            pltpu.VMEM(metric.shape, BF),
            pltpu.VMEM(active.shape, BF),
            pltpu.VMEM((LANES * pitch, LANES), F32),
            pltpu.VMEM((span, acts * pairs), BF),
            pltpu.SemaphoreType.DMA((3,)),
        ],
        compiler_params=pltpu.CompilerParams(vmem_limit_bytes=PACK_LIMIT),
    )(*(pltpu.with_memory_space_constraint(a, pltpu.HBM) for a in (x, metric, active)))


def pieces(item, pairs):
    first, end = item * pairs, (item + 1) * pairs
    return [
        (k, max(first, k * USED) - first, min(end, (k + 1) * USED) - first)
        for k in range(first // USED, (end - 1) // USED + 1)
    ]


def parts(chunk, pairs):
    first, end = chunk * USED, (chunk + 1) * USED
    return [
        (i, max(first, i * pairs) - first, min(end, (i + 1) * pairs) - first)
        for i in range(first // pairs, (end - 1) // pairs + 1)
    ]


def turned(tile, shift):
    shift %= LANES
    return tile if shift == 0 else pltpu.roll(tile, shift, 1)


def joined(found, lane):
    tile = found[0][0]
    for other, first in found[1:]:
        tile = jnp.where(lane >= first, other, tile)
    return tile


def place(j, v, count):
    return (j * 2 + v % 2) * (count // 2) + v // 2


def mid_kernel(acts, rows, pairs, items, r_ref, f_ref, wide_ref, out_ref, flat, u_ref, y_ref):
    count = r_ref.shape[0] // acts
    tall = count * rows
    chunks = pairs * items // USED
    used = chunks * rows
    lane = lax.broadcasted_iota(jnp.int32, (tall, LANES), 1)
    for j in range(acts):
        for v in range(count):
            block = r_ref[place(j, v, count)].astype(F32)
            for k in range(chunks):
                flat[0, v * rows : (v + 1) * rows, k * LANES : (k + 1) * LANES] = block[k * rows : (k + 1) * rows]
        for i in range(items):
            found = [
                (turned(flat[0, :, k * LANES : (k + 1) * LANES], k * USED - i * pairs), first)
                for k, first, end in pieces(i, pairs)
            ]
            u_ref[i, :, j * LANES : (j + 1) * LANES] = joined(found, lane).astype(BF)
    for i in range(items):
        y_ref[i] = jnp.dot(u_ref[i], wide_ref[...], preferred_element_type=F32)
    for j in range(acts):
        for n in range(2):
            at = (n * acts + j) * LANES
            for k in range(chunks):
                found = [
                    (turned(y_ref[i, :, at : at + LANES], i * pairs - k * USED), first)
                    for i, first, end in parts(k, pairs)
                ]
                flat[n, :, k * LANES : (k + 1) * LANES] = joined(found, lane)
        flat[1] = flat[1] + jnp.dot(f_ref[...], flat[0].astype(BF), preferred_element_type=F32)
        for n in range(2):
            for v in range(count):
                block = jnp.concatenate(
                    [flat[n, v * rows : (v + 1) * rows, k * LANES : (k + 1) * LANES] for k in range(chunks)],
                    axis=0,
                )
                out_ref[place(j, v, count), n * used : (n + 1) * used, :] = block.astype(BF)


def middle(received, fock, wide, acts, rows, pairs, items):
    count = received.shape[0] // acts
    tall = count * rows
    chunks = pairs * items // USED
    vmem = pl.BlockSpec(memory_space=pltpu.VMEM)
    return pl.pallas_call(
        functools.partial(mid_kernel, acts, rows, pairs, items),
        out_shape=jax.ShapeDtypeStruct((LANES, 2 * chunks * rows, LANES), BF),
        in_specs=[vmem] * 3,
        out_specs=vmem,
        scratch_shapes=[
            pltpu.VMEM((2, tall, chunks * LANES), F32),
            pltpu.VMEM((items, tall, acts * LANES), BF),
            pltpu.VMEM((items, tall, 2 * acts * LANES), F32),
        ],
        compiler_params=pltpu.CompilerParams(vmem_limit_bytes=MID_LIMIT),
    )(received, fock, wide)


def last_kernel(pitch, r_ref, x_ref, f_ref, s_all, w_all, sums_ref, scratch):
    rows, pairs, width = x_ref.shape
    items = width // LANES
    chunks = pairs * items // USED
    used = chunks * rows
    group, tall = w_all.shape[0] // LANES_ROWS, LANES_ROWS
    whole = pairs // 8 * 8
    for d in range(LANES):
        scratch[d * pitch : d * pitch + 2 * used, :] = r_ref[d].astype(F32)
    sel = [
        jnp.concatenate(
            [onehot((tall, LANES), i * pairs, k * USED, pairs, USED) for k, first, end in pieces(i, pairs)],
            axis=1,
        )
        for i in range(items)
    ]
    sums = [jnp.zeros((8, width), F32)] * 5
    for base in range(0, rows, group):
        for a in range(0, group, 2):
            for n, target in enumerate((w_all, s_all)):
                got = [
                    jnp.concatenate(
                        [
                            scratch[pl.ds(n * used + k * rows + base + b, LANES, stride=pitch), :]
                            for b in (a, a + 1)
                        ],
                        axis=0,
                    ).astype(BF)
                    for k in range(chunks)
                ]
                for i in range(items):
                    source = jnp.concatenate([got[k] for k, first, end in pieces(i, pairs)], axis=1)
                    both = lax.dot_general(sel[i], source, NT_DIMS, preferred_element_type=F32)
                    both = both.astype(target.dtype)
                    for b in range(2):
                        target[(a + b) * tall : (a + b + 1) * tall, i * LANES : (i + 1) * LANES] = both[
                            :, b * LANES : (b + 1) * LANES
                        ]
        s_all[...] = s_all[...] + jnp.dot(w_all[...], f_ref[...], preferred_element_type=F32)
        for a in range(group):
            for first, end in ((0, whole), (whole, pairs)):
                x = x_ref[base + a, first:end].astype(F32)
                w = w_all[a * tall + first : a * tall + end, :].astype(F32)
                s = s_all[a * tall + first : a * tall + end, :]
                for n, product in enumerate((x * s, x * w, s * s, s * w, w * w)):
                    if end - first >= 8:
                        product = jnp.sum(product.reshape(-1, 8, width), axis=0)
                    else:
                        product = jnp.concatenate(
                            [product, jnp.zeros((8 - (end - first), width), F32)], axis=0
                        )
                    sums[n] = sums[n] + product
    lane = lax.broadcasted_iota(jnp.int32, (1, LANES), 1)
    packed = jnp.zeros((1, LANES), F32)
    for n in range(5):
        packed = packed + jnp.where(lane == n, jnp.sum(sums[n]), 0.0)
    for d in range(sums_ref.shape[0]):
        sums_ref[d] = packed


def last(received, x, fock):
    rows, pairs, width = x.shape
    used = received.shape[1] // 2
    pitch = 2 * used + 8
    vmem = pl.BlockSpec(memory_space=pltpu.VMEM)
    return pl.pallas_call(
        functools.partial(last_kernel, pitch),
        out_shape=(
            jax.ShapeDtypeStruct((rows * LANES_ROWS, width), F32),
            jax.ShapeDtypeStruct((rows * LANES_ROWS, width), BF),
            jax.ShapeDtypeStruct((LANES, 1, LANES), F32),
        ),
        in_specs=[vmem] * 3,
        out_specs=(vmem, vmem, vmem),
        scratch_shapes=[
            pltpu.VMEM((LANES * pitch, LANES), F32),
        ],
        compiler_params=pltpu.CompilerParams(vmem_limit_bytes=LAST_LIMIT),
    )(received, x, fock)


def finish_kernel(sums_ref, sigma_ref, w_ref, resid_hbm, ratio_ref, norm_ref, resid_ref, sems):
    totals = jnp.sum(sums_ref[...], axis=0)
    lane = lax.broadcasted_iota(jnp.int32, totals.shape, 1)
    total = [jnp.sum(jnp.where(lane == n, totals, 0.0)) for n in range(5)]
    rayleigh = jnp.full((1, LANES), total[0]) / jnp.full((1, LANES), total[1])
    squares = total[2] - 2.0 * rayleigh * total[3] + rayleigh * rayleigh * total[4]
    ratio_ref[...] = rayleigh
    norm_ref[...] = squares / jnp.full((1, LANES), total[1])
    rows, pairs, width = resid_ref.shape
    wide = jnp.concatenate([rayleigh] * (width // LANES), axis=1)
    group = rows // sems.shape[0]
    copies = []
    for a in range(rows):
        some = slice(a * LANES_ROWS, a * LANES_ROWS + pairs)
        resid_ref[a] = (sigma_ref[some] - wide * w_ref[some].astype(F32)).astype(BF)
        if (a + 1) % group == 0:
            part = pl.ds(a + 1 - group, group)
            copies.append(pltpu.make_async_copy(resid_ref.at[part], resid_hbm.at[part], sems.at[a // group]))
            copies[-1].start()
    for copy in copies:
        copy.wait()


def finish(sums, sigma, weighted, shape):
    vmem = pl.BlockSpec(memory_space=pltpu.VMEM)
    row = jax.ShapeDtypeStruct((1, LANES), F32)
    return pl.pallas_call(
        finish_kernel,
        out_shape=(jax.ShapeDtypeStruct(shape, BF), row, row),
        in_specs=[vmem] * 3,
        out_specs=(pl.BlockSpec(memory_space=pltpu.HBM), vmem, vmem),
        scratch_shapes=[pltpu.VMEM(shape, BF), pltpu.SemaphoreType.DMA((5,))],
        compiler_params=pltpu.CompilerParams(vmem_limit_bytes=FINISH_LIMIT),
    )(sums, sigma, weighted)


def exchange(value):
    return lax.all_to_all(value, ALL, split_axis=0, concat_axis=0, tiled=True)


def local(amplitudes, virtual_fock_block, metric, active_block):
    acts = lax.axis_size("act")
    x = jnp.transpose(amplitudes, (1, 0, 2))
    rows, pairs, width = x.shape
    items = width // LANES
    packed, wide = pack(x, metric, active_block, acts)
    arrived = exchange(packed)
    sent = middle(arrived, virtual_fock_block, wide, acts, rows, pairs, items)
    sigma, weighted, partial = last(exchange(sent), x, virtual_fock_block)
    resid, rayleigh, norm = finish(exchange(partial), sigma, weighted, x.shape)
    return jnp.transpose(resid, (1, 0, 2)), rayleigh[0, 0], norm[0, 0]


def solution(mesh):
    acts, virts = mesh.shape["act"], mesh.shape["virt"]
    torus = Mesh(mesh.devices.reshape(acts, 4, virts // 8, 2), ("act",) + VIRT)
    in_specs = (P("act", VIRT, None), P(), P(), P())
    out_specs = (P("act", VIRT, None), P(), P())
    return jax.shard_map(local, mesh=torus, in_specs=in_specs, out_specs=out_specs, check_vma=False)
```

```python
import functools

import jax
import jax.numpy as jnp
from jax import lax
from jax.experimental import pallas as pl
from jax.experimental.pallas import tpu as pltpu
from jax.sharding import Mesh
from jax.sharding import PartitionSpec as P

BF = jnp.bfloat16
F32 = jnp.float32
VIRT = ("virt_0", "virt_1", "core")
ALL = ("act", "core", "virt_0", "virt_1")
LANES = 128
USED = 125
MIB = 1024 * 1024
PACK_LIMIT, MID_LIMIT, LAST_LIMIT, FINISH_LIMIT = 16 * MIB, 26 * MIB, 32 * MIB, 8 * MIB
LANES_ROWS = 104
NT_DIMS = (((1,), (1,)), ((), ()))
TN_DIMS = (((0,), (0,)), ((), ()))


def onehot(shape, row_base, column_base, row_end, column_end):
    rows = lax.broadcasted_iota(jnp.int32, shape, 0)
    columns = lax.broadcasted_iota(jnp.int32, shape, 1)
    same = (rows + row_base) == (columns + column_base)
    keep = same & (rows < row_end) & (columns < column_end)
    return jnp.where(keep, 1.0, 0.0).astype(BF)


def touching(pairs, items):
    chunks = pairs * items // USED
    return [
        [i for i in range(items) if i * pairs < (k + 1) * USED and (i + 1) * pairs > k * USED]
        for k in range(chunks)
    ]


def pack_kernel(acts, pitch, x_hbm, m_hbm, h_hbm, out_ref, wide_ref, x_ref, m_ref, h_ref, scratch, padded, sems):
    rows, pairs, width = x_hbm.shape
    items = width // LANES
    table = touching(pairs, items)
    chunks = len(table)
    pairs_of = ((m_hbm, m_ref), (h_hbm, h_ref), (x_hbm, x_ref))
    copies = [pltpu.make_async_copy(a, b, sems.at[n]) for n, (a, b) in enumerate(pairs_of)]
    for copy in copies:
        copy.start()
    span = acts * LANES
    for j in range(acts):
        padded[j * LANES : (j + 1) * LANES, :] = onehot((LANES, acts * pairs), j * pairs, 0, pairs, acts * pairs)
    for n, matrix in enumerate((m_ref, h_ref)):
        copies[n].wait()
        half = lax.dot_general(padded[...], matrix[...], NT_DIMS, preferred_element_type=F32).astype(BF)
        wide = lax.dot_general(half, padded[...], NT_DIMS, preferred_element_type=F32)
        wide_ref[:, n * span : (n + 1) * span] = wide.astype(BF)
    sel = {
        (k, i): onehot((pairs, LANES), i * pairs, k * USED, pairs, USED)
        for k in range(chunks)
        for i in table[k]
    }
    copies[2].wait()
    for a in range(rows):
        for k in range(chunks):
            total = None
            for i in table[k]:
                part = lax.dot_general(
                    x_ref[a, :, i * LANES : (i + 1) * LANES], sel[k, i], TN_DIMS, preferred_element_type=F32
                )
                total = part if total is None else total + part
            scratch[pl.ds(k * rows + a, LANES, stride=pitch), :] = total
    used = chunks * rows
    for d in range(LANES):
        out_ref[d] = scratch[d * pitch : d * pitch + used, :].astype(BF)


def pack(x, metric, active, acts):
    rows, pairs, width = x.shape
    used = pairs * (width // LANES) // USED * rows
    pitch = used + 8
    span = acts * LANES
    vmem = pl.BlockSpec(memory_space=pltpu.VMEM)
    return pl.pallas_call(
        functools.partial(pack_kernel, acts, pitch),
        out_shape=(
            jax.ShapeDtypeStruct((LANES, used, LANES), BF),
            jax.ShapeDtypeStruct((span, 2 * span), BF),
        ),
        in_specs=[pl.BlockSpec(memory_space=pltpu.HBM)] * 3,
        out_specs=(vmem, vmem),
        scratch_shapes=[
            pltpu.VMEM(x.shape, BF),
            pltpu.VMEM(metric.shape, BF),
            pltpu.VMEM(active.shape, BF),
            pltpu.VMEM(((LANES + 1) * pitch, LANES), F32),
            pltpu.VMEM((span, acts * pairs), BF),
            pltpu.SemaphoreType.DMA((3,)),
        ],
        compiler_params=pltpu.CompilerParams(vmem_limit_bytes=PACK_LIMIT),
    )(*(pltpu.with_memory_space_constraint(a, pltpu.HBM) for a in (x, metric, active)))


def pieces(item, pairs):
    first, end = item * pairs, (item + 1) * pairs
    return [
        (k, max(first, k * USED) - first, min(end, (k + 1) * USED) - first)
        for k in range(first // USED, (end - 1) // USED + 1)
    ]


def parts(chunk, pairs):
    first, end = chunk * USED, (chunk + 1) * USED
    return [
        (i, max(first, i * pairs) - first, min(end, (i + 1) * pairs) - first)
        for i in range(first // pairs, (end - 1) // pairs + 1)
    ]


def turned(tile, shift):
    shift %= LANES
    return tile if shift == 0 else pltpu.roll(tile, shift, 1)


def joined(found, lane):
    tile = found[0][0]
    for other, first in found[1:]:
        tile = jnp.where(lane >= first, other, tile)
    return tile


def place(j, v, count):
    return (j * 2 + v % 2) * (count // 2) + v // 2


def mid_kernel(acts, rows, pairs, items, r_ref, f_ref, wide_ref, out_ref, flat, u_ref, y_ref):
    count = r_ref.shape[0] // acts
    tall = count * rows
    chunks = pairs * items // USED
    used = chunks * rows
    lane = lax.broadcasted_iota(jnp.int32, (tall, LANES), 1)
    for j in range(acts):
        for v in range(count):
            block = r_ref[place(j, v, count)].astype(F32)
            for k in range(chunks):
                flat[0, v * rows : (v + 1) * rows, k * LANES : (k + 1) * LANES] = block[k * rows : (k + 1) * rows]
        for i in range(items):
            found = [
                (turned(flat[0, :tall, k * LANES : (k + 1) * LANES], k * USED - i * pairs), first)
                for k, first, end in pieces(i, pairs)
            ]
            u_ref[i, :, j * LANES : (j + 1) * LANES] = joined(found, lane).astype(BF)
    for i in range(items):
        y_ref[i] = jnp.dot(u_ref[i], wide_ref[...], preferred_element_type=F32)
    for j in range(acts):
        for n in range(2):
            at = (n * acts + j) * LANES
            for k in range(chunks):
                found = [
                    (turned(y_ref[i, :, at : at + LANES], i * pairs - k * USED), first)
                    for i, first, end in parts(k, pairs)
                ]
                flat[n, :tall, k * LANES : (k + 1) * LANES] = joined(found, lane)
        right = jnp.dot(f_ref[...], flat[0, :tall].astype(BF), preferred_element_type=F32)
        flat[1, :tall] = flat[1, :tall] + right
        for n in range(2):
            for v in range(count):
                block = jnp.concatenate(
                    [flat[n, v * rows : (v + 1) * rows, k * LANES : (k + 1) * LANES] for k in range(chunks)],
                    axis=0,
                )
                out_ref[place(j, v, count), n * used : (n + 1) * used, :] = block.astype(BF)


def middle(received, fock, wide, acts, rows, pairs, items):
    count = received.shape[0] // acts
    tall = count * rows
    chunks = pairs * items // USED
    vmem = pl.BlockSpec(memory_space=pltpu.VMEM)
    return pl.pallas_call(
        functools.partial(mid_kernel, acts, rows, pairs, items),
        out_shape=jax.ShapeDtypeStruct((LANES, 2 * chunks * rows, LANES), BF),
        in_specs=[vmem] * 3,
        out_specs=vmem,
        scratch_shapes=[
            pltpu.VMEM((2, tall + 8, chunks * LANES), F32),
            pltpu.VMEM((items, tall, acts * LANES), BF),
            pltpu.VMEM((items, tall, 2 * acts * LANES), F32),
        ],
        compiler_params=pltpu.CompilerParams(vmem_limit_bytes=MID_LIMIT),
    )(received, fock, wide)


def last_kernel(pitch, r_ref, x_ref, f_ref, s_all, w_all, sums_ref, scratch):
    rows, pairs, width = x_ref.shape
    items = width // LANES
    chunks = pairs * items // USED
    used = chunks * rows
    group, tall = w_all.shape[0] // LANES_ROWS, LANES_ROWS
    whole = pairs // 8 * 8
    for d in range(LANES):
        scratch[d * pitch : d * pitch + 2 * used, :] = r_ref[d].astype(F32)
    covers = [((k, k + 1), []) for k in range(0, chunks, 2)]
    for i in range(items):
        need = tuple(k for k, first, end in pieces(i, pairs))
        fits = [served for held, served in covers if set(need) <= set(held)]
        if fits:
            fits[0].append(i)
        else:
            covers.append((need, [i]))
    sel = [
        jnp.concatenate(
            [
                jnp.concatenate([onehot((tall, LANES), i * pairs, k * USED, pairs, USED) for k in held], axis=1)
                for i in served
            ],
            axis=0,
        )
        for held, served in covers
    ]
    sums = [jnp.zeros((8, width), F32)] * 5
    for base in range(0, rows, group):
        for a in range(0, group, 2):
            for n, target in enumerate((w_all, s_all)):
                got = [
                    jnp.concatenate(
                        [
                            scratch[pl.ds(n * used + k * rows + base + b, LANES, stride=pitch), :]
                            for b in (a, a + 1)
                        ],
                        axis=0,
                    ).astype(BF)
                    for k in range(chunks)
                ]
                for rows_of, (held, served) in zip(sel, covers):
                    source = jnp.concatenate([got[k] for k in held], axis=1)
                    both = lax.dot_general(rows_of, source, NT_DIMS, preferred_element_type=F32)
                    both = both.astype(target.dtype)
                    for n_item, i in enumerate(served):
                        for b in range(2):
                            target[(a + b) * tall : (a + b + 1) * tall, i * LANES : (i + 1) * LANES] = both[
                                n_item * tall : (n_item + 1) * tall, b * LANES : (b + 1) * LANES
                            ]
        s_all[...] = s_all[...] + jnp.dot(w_all[...], f_ref[...], preferred_element_type=F32)
        for a in range(group):
            for first, end in ((0, whole), (whole, pairs)):
                x = x_ref[base + a, first:end].astype(F32)
                w = w_all[a * tall + first : a * tall + end, :].astype(F32)
                s = s_all[a * tall + first : a * tall + end, :]
                for n, product in enumerate((x * s, x * w, s * s, s * w, w * w)):
                    if end - first >= 8:
                        product = jnp.sum(product.reshape(-1, 8, width), axis=0)
                    else:
                        product = jnp.concatenate(
                            [product, jnp.zeros((8 - (end - first), width), F32)], axis=0
                        )
                    sums[n] = sums[n] + product
    lane = lax.broadcasted_iota(jnp.int32, (1, LANES), 1)
    packed = jnp.zeros((1, LANES), F32)
    for n in range(5):
        packed = packed + jnp.where(lane == n, jnp.sum(sums[n]), 0.0)
    for d in range(sums_ref.shape[0]):
        sums_ref[d] = packed


def last(received, x, fock):
    rows, pairs, width = x.shape
    used = received.shape[1] // 2
    pitch = 2 * used + 8
    vmem = pl.BlockSpec(memory_space=pltpu.VMEM)
    return pl.pallas_call(
        functools.partial(last_kernel, pitch),
        out_shape=(
            jax.ShapeDtypeStruct((rows * LANES_ROWS, width), F32),
            jax.ShapeDtypeStruct((rows * LANES_ROWS, width), BF),
            jax.ShapeDtypeStruct((LANES, 1, LANES), F32),
        ),
        in_specs=[vmem] * 3,
        out_specs=(vmem, vmem, vmem),
        scratch_shapes=[
            pltpu.VMEM(((LANES + 1) * pitch, LANES), F32),
        ],
        compiler_params=pltpu.CompilerParams(vmem_limit_bytes=LAST_LIMIT),
    )(received, x, fock)


def finish_kernel(sums_ref, sigma_ref, w_ref, resid_hbm, ratio_ref, norm_ref, resid_ref, sems):
    totals = jnp.sum(sums_ref[...], axis=0)
    lane = lax.broadcasted_iota(jnp.int32, totals.shape, 1)
    total = [jnp.sum(jnp.where(lane == n, totals, 0.0)) for n in range(5)]
    rayleigh = jnp.full((1, LANES), total[0]) / jnp.full((1, LANES), total[1])
    squares = total[2] - 2.0 * rayleigh * total[3] + rayleigh * rayleigh * total[4]
    ratio_ref[...] = rayleigh
    norm_ref[...] = squares / jnp.full((1, LANES), total[1])
    rows, pairs, width = resid_ref.shape
    wide = jnp.concatenate([rayleigh] * (width // LANES), axis=1)
    group = rows // sems.shape[0]
    copies = []
    for a in range(rows):
        some = slice(a * LANES_ROWS, a * LANES_ROWS + pairs)
        resid_ref[a] = (sigma_ref[some] - wide * w_ref[some].astype(F32)).astype(BF)
        if (a + 1) % group == 0:
            part = pl.ds(a + 1 - group, group)
            copies.append(pltpu.make_async_copy(resid_ref.at[part], resid_hbm.at[part], sems.at[a // group]))
            copies[-1].start()
    for copy in copies:
        copy.wait()


def finish(sums, sigma, weighted, shape):
    vmem = pl.BlockSpec(memory_space=pltpu.VMEM)
    row = jax.ShapeDtypeStruct((1, LANES), F32)
    return pl.pallas_call(
        finish_kernel,
        out_shape=(jax.ShapeDtypeStruct(shape, BF), row, row),
        in_specs=[vmem] * 3,
        out_specs=(pl.BlockSpec(memory_space=pltpu.HBM), vmem, vmem),
        scratch_shapes=[pltpu.VMEM(shape, BF), pltpu.SemaphoreType.DMA((10,))],
        compiler_params=pltpu.CompilerParams(vmem_limit_bytes=FINISH_LIMIT),
    )(sums, sigma, weighted)


def exchange(value):
    return lax.all_to_all(value, ALL, split_axis=0, concat_axis=0, tiled=True)


def local(amplitudes, virtual_fock_block, metric, active_block):
    acts = lax.axis_size("act")
    x = jnp.transpose(amplitudes, (1, 0, 2))
    rows, pairs, width = x.shape
    items = width // LANES
    packed, wide = pack(x, metric, active_block, acts)
    arrived = exchange(packed)
    sent = middle(arrived, virtual_fock_block, wide, acts, rows, pairs, items)
    sigma, weighted, partial = last(exchange(sent), x, virtual_fock_block)
    resid, rayleigh, norm = finish(exchange(partial), sigma, weighted, x.shape)
    return jnp.transpose(resid, (1, 0, 2)), rayleigh[0, 0], norm[0, 0]


def solution(mesh):
    acts, virts = mesh.shape["act"], mesh.shape["virt"]
    torus = Mesh(mesh.devices.reshape(acts, 4, virts // 8, 2), ("act",) + VIRT)
    in_specs = (P("act", VIRT, None), P(), P(), P())
    out_specs = (P("act", VIRT, None), P(), P())
    return jax.shard_map(local, mesh=torus, in_specs=in_specs, out_specs=out_specs, check_vma=False)
```

```python
import functools

import jax
import jax.numpy as jnp
from jax import lax
from jax.experimental import pallas as pl
from jax.experimental.pallas import tpu as pltpu
from jax.sharding import Mesh
from jax.sharding import PartitionSpec as P

BF = jnp.bfloat16
F32 = jnp.float32
VIRT = ("virt_0", "virt_1", "core")
ALL = ("act", "core", "virt_0", "virt_1")
LANES = 128
USED = 125
MIB = 1024 * 1024
PACK_LIMIT, MID_LIMIT, LAST_LIMIT, FINISH_LIMIT = 16 * MIB, 26 * MIB, 32 * MIB, 8 * MIB
LANES_ROWS = 104
NT_DIMS = (((1,), (1,)), ((), ()))
TN_DIMS = (((0,), (0,)), ((), ()))


def onehot(shape, row_base, column_base, row_end, column_end):
    rows = lax.broadcasted_iota(jnp.int32, shape, 0)
    columns = lax.broadcasted_iota(jnp.int32, shape, 1)
    same = (rows + row_base) == (columns + column_base)
    keep = same & (rows < row_end) & (columns < column_end)
    return jnp.where(keep, 1.0, 0.0).astype(BF)


def touching(pairs, items):
    chunks = pairs * items // USED
    return [
        [i for i in range(items) if i * pairs < (k + 1) * USED and (i + 1) * pairs > k * USED]
        for k in range(chunks)
    ]


def pack_kernel(acts, pitch, x_hbm, m_hbm, h_hbm, out_ref, wide_ref, x_ref, m_ref, h_ref, scratch, padded, sems):
    rows, pairs, width = x_hbm.shape
    items = width // LANES
    table = touching(pairs, items)
    chunks = len(table)
    pairs_of = ((m_hbm, m_ref), (h_hbm, h_ref), (x_hbm, x_ref))
    copies = [pltpu.make_async_copy(a, b, sems.at[n]) for n, (a, b) in enumerate(pairs_of)]
    for copy in copies:
        copy.start()
    span = acts * LANES
    for j in range(acts):
        padded[j * LANES : (j + 1) * LANES, :] = onehot((LANES, acts * pairs), j * pairs, 0, pairs, acts * pairs)
    for n, matrix in enumerate((m_ref, h_ref)):
        copies[n].wait()
        half = lax.dot_general(padded[...], matrix[...], NT_DIMS, preferred_element_type=F32).astype(BF)
        wide = lax.dot_general(half, padded[...], NT_DIMS, preferred_element_type=F32)
        wide_ref[:, n * span : (n + 1) * span] = wide.astype(BF)
    sel = {
        (k, i): onehot((pairs, LANES), i * pairs, k * USED, pairs, USED)
        for k in range(chunks)
        for i in table[k]
    }
    copies[2].wait()
    for a in range(rows):
        for k in range(chunks):
            total = None
            for i in table[k]:
                part = lax.dot_general(
                    x_ref[a, :, i * LANES : (i + 1) * LANES], sel[k, i], TN_DIMS, preferred_element_type=F32
                )
                total = part if total is None else total + part
            scratch[pl.ds(k * rows + a, LANES, stride=pitch), :] = total
    used = chunks * rows
    for d in range(LANES):
        out_ref[d] = scratch[d * pitch : d * pitch + used, :].astype(BF)


def pack(x, metric, active, acts):
    rows, pairs, width = x.shape
    used = pairs * (width // LANES) // USED * rows
    pitch = used + 8
    span = acts * LANES
    vmem = pl.BlockSpec(memory_space=pltpu.VMEM)
    return pl.pallas_call(
        functools.partial(pack_kernel, acts, pitch),
        out_shape=(
            jax.ShapeDtypeStruct((LANES, used, LANES), BF),
            jax.ShapeDtypeStruct((span, 2 * span), BF),
        ),
        in_specs=[pl.BlockSpec(memory_space=pltpu.HBM)] * 3,
        out_specs=(vmem, vmem),
        scratch_shapes=[
            pltpu.VMEM(x.shape, BF),
            pltpu.VMEM(metric.shape, BF),
            pltpu.VMEM(active.shape, BF),
            pltpu.VMEM(((LANES + 1) * pitch, LANES), F32),
            pltpu.VMEM((span, acts * pairs), BF),
            pltpu.SemaphoreType.DMA((3,)),
        ],
        compiler_params=pltpu.CompilerParams(vmem_limit_bytes=PACK_LIMIT),
    )(*(pltpu.with_memory_space_constraint(a, pltpu.HBM) for a in (x, metric, active)))


def pieces(item, pairs):
    first, end = item * pairs, (item + 1) * pairs
    return [
        (k, max(first, k * USED) - first, min(end, (k + 1) * USED) - first)
        for k in range(first // USED, (end - 1) // USED + 1)
    ]


def parts(chunk, pairs):
    first, end = chunk * USED, (chunk + 1) * USED
    return [
        (i, max(first, i * pairs) - first, min(end, (i + 1) * pairs) - first)
        for i in range(first // pairs, (end - 1) // pairs + 1)
    ]


def turned(tile, shift):
    shift %= LANES
    return tile if shift == 0 else pltpu.roll(tile, shift, 1)


def joined(found, lane):
    tile = found[0][0]
    for other, first in found[1:]:
        tile = jnp.where(lane >= first, other, tile)
    return tile


def place(j, v, count):
    return (j * 2 + v % 2) * (count // 2) + v // 2


def mid_kernel(acts, rows, pairs, items, r_ref, f_ref, wide_ref, out_ref, flat, u_ref, y_ref):
    count = r_ref.shape[0] // acts
    tall = count * rows
    chunks = pairs * items // USED
    used = chunks * rows
    lane = lax.broadcasted_iota(jnp.int32, (tall, LANES), 1)
    for j in range(acts):
        for v in range(count):
            block = r_ref[place(j, v, count)].astype(F32)
            for k in range(chunks):
                flat[0, v * rows : (v + 1) * rows, k * LANES : (k + 1) * LANES] = block[k * rows : (k + 1) * rows]
        for i in range(items):
            found = [
                (turned(flat[0, :tall, k * LANES : (k + 1) * LANES], k * USED - i * pairs), first)
                for k, first, end in pieces(i, pairs)
            ]
            u_ref[i, :, j * LANES : (j + 1) * LANES] = joined(found, lane).astype(BF)
    for i in range(items):
        y_ref[i] = jnp.dot(u_ref[i], wide_ref[...], preferred_element_type=F32)
    for j in range(acts):
        for n in range(2):
            at = (n * acts + j) * LANES
            for k in range(chunks):
                found = [
                    (turned(y_ref[i, :, at : at + LANES], i * pairs - k * USED), first)
                    for i, first, end in parts(k, pairs)
                ]
                flat[n, :tall, k * LANES : (k + 1) * LANES] = joined(found, lane)
        right = jnp.dot(f_ref[...], flat[0, :tall].astype(BF), preferred_element_type=F32)
        flat[1, :tall] = flat[1, :tall] + right
        for n in range(2):
            for v in range(count):
                block = jnp.concatenate(
                    [flat[n, v * rows : (v + 1) * rows, k * LANES : (k + 1) * LANES] for k in range(chunks)],
                    axis=0,
                )
                out_ref[place(j, v, count), n * used : (n + 1) * used, :] = block.astype(BF)


def middle(received, fock, wide, acts, rows, pairs, items):
    count = received.shape[0] // acts
    tall = count * rows
    chunks = pairs * items // USED
    vmem = pl.BlockSpec(memory_space=pltpu.VMEM)
    return pl.pallas_call(
        functools.partial(mid_kernel, acts, rows, pairs, items),
        out_shape=jax.ShapeDtypeStruct((LANES, 2 * chunks * rows, LANES), BF),
        in_specs=[vmem] * 3,
        out_specs=vmem,
        scratch_shapes=[
            pltpu.VMEM((2, tall + 8, chunks * LANES), F32),
            pltpu.VMEM((items, tall, acts * LANES), BF),
            pltpu.VMEM((items, tall, 2 * acts * LANES), F32),
        ],
        compiler_params=pltpu.CompilerParams(vmem_limit_bytes=MID_LIMIT),
    )(received, fock, wide)


def last_kernel(pitch, r_ref, x_ref, f_ref, s_all, w_all, sums_ref, scratch):
    rows, pairs, width = x_ref.shape
    items = width // LANES
    chunks = pairs * items // USED
    used = chunks * rows
    group, tall = w_all.shape[0] // LANES_ROWS, LANES_ROWS
    whole = pairs // 8 * 8
    for d in range(LANES):
        scratch[d * pitch : d * pitch + 2 * used, :] = r_ref[d].astype(F32)
    covers = [((k, k + 1), []) for k in range(0, chunks, 2)]
    for i in range(items):
        need = tuple(k for k, first, end in pieces(i, pairs))
        fits = [served for held, served in covers if set(need) <= set(held)]
        if fits:
            fits[0].append(i)
        else:
            covers.append((need, [i]))
    sel = [
        jnp.concatenate(
            [
                jnp.concatenate([onehot((tall, LANES), i * pairs, k * USED, pairs, USED) for k in held], axis=1)
                for i in served
            ],
            axis=0,
        )
        for held, served in covers
    ]
    sums = [jnp.zeros((8, width), F32)] * 5
    for base in range(0, rows, group):
        for a in range(0, group, 2):
            for n, target in enumerate((w_all, s_all)):
                got = [
                    jnp.concatenate(
                        [
                            scratch[pl.ds(n * used + k * rows + base + b, LANES, stride=pitch), :]
                            for b in (a, a + 1)
                        ],
                        axis=0,
                    ).astype(BF)
                    for k in range(chunks)
                ]
                for rows_of, (held, served) in zip(sel, covers):
                    source = jnp.concatenate([got[k] for k in held], axis=1)
                    both = lax.dot_general(rows_of, source, NT_DIMS, preferred_element_type=F32)
                    both = both.astype(target.dtype)
                    for n_item, i in enumerate(served):
                        for b in range(2):
                            target[(a + b) * tall : (a + b + 1) * tall, i * LANES : (i + 1) * LANES] = both[
                                n_item * tall : (n_item + 1) * tall, b * LANES : (b + 1) * LANES
                            ]
        s_all[...] = s_all[...] + jnp.dot(w_all[...], f_ref[...], preferred_element_type=F32)
        for a in range(group):
            for first, end in ((0, whole), (whole, pairs)):
                x = x_ref[base + a, first:end].astype(F32)
                w = w_all[a * tall + first : a * tall + end, :].astype(F32)
                s = s_all[a * tall + first : a * tall + end, :]
                for n, product in enumerate((x * s, x * w, s * s, s * w, w * w)):
                    if end - first >= 8:
                        product = jnp.sum(product.reshape(-1, 8, width), axis=0)
                    else:
                        product = jnp.concatenate(
                            [product, jnp.zeros((8 - (end - first), width), F32)], axis=0
                        )
                    sums[n] = sums[n] + product
    lane = lax.broadcasted_iota(jnp.int32, (1, LANES), 1)
    packed = jnp.zeros((1, LANES), F32)
    for n in range(5):
        packed = packed + jnp.where(lane == n, jnp.sum(sums[n]), 0.0)
    for d in range(sums_ref.shape[0]):
        sums_ref[d] = packed


def last(received, x, fock):
    rows, pairs, width = x.shape
    used = received.shape[1] // 2
    pitch = 2 * used + 4
    vmem = pl.BlockSpec(memory_space=pltpu.VMEM)
    return pl.pallas_call(
        functools.partial(last_kernel, pitch),
        out_shape=(
            jax.ShapeDtypeStruct((rows * LANES_ROWS, width), F32),
            jax.ShapeDtypeStruct((rows * LANES_ROWS, width), BF),
            jax.ShapeDtypeStruct((LANES, 1, LANES), F32),
        ),
        in_specs=[vmem] * 3,
        out_specs=(vmem, vmem, vmem),
        scratch_shapes=[
            pltpu.VMEM(((LANES + 1) * pitch, LANES), F32),
        ],
        compiler_params=pltpu.CompilerParams(vmem_limit_bytes=LAST_LIMIT),
    )(received, x, fock)


def finish_kernel(sums_ref, sigma_ref, w_ref, resid_hbm, ratio_ref, norm_ref, resid_ref, sems):
    totals = jnp.sum(sums_ref[...], axis=0)
    lane = lax.broadcasted_iota(jnp.int32, totals.shape, 1)
    total = [jnp.sum(jnp.where(lane == n, totals, 0.0)) for n in range(5)]
    rayleigh = jnp.full((1, LANES), total[0]) / jnp.full((1, LANES), total[1])
    squares = total[2] - 2.0 * rayleigh * total[3] + rayleigh * rayleigh * total[4]
    ratio_ref[...] = rayleigh
    norm_ref[...] = squares / jnp.full((1, LANES), total[1])
    rows, pairs, width = resid_ref.shape
    wide = jnp.concatenate([rayleigh] * (width // LANES), axis=1)
    group = rows // sems.shape[0]
    copies = []
    for a in range(rows):
        some = slice(a * LANES_ROWS, a * LANES_ROWS + pairs)
        resid_ref[a] = (sigma_ref[some] - wide * w_ref[some].astype(F32)).astype(BF)
        if (a + 1) % group == 0:
            part = pl.ds(a + 1 - group, group)
            copies.append(pltpu.make_async_copy(resid_ref.at[part], resid_hbm.at[part], sems.at[a // group]))
            copies[-1].start()
    for copy in copies:
        copy.wait()


def finish(sums, sigma, weighted, shape):
    vmem = pl.BlockSpec(memory_space=pltpu.VMEM)
    row = jax.ShapeDtypeStruct((1, LANES), F32)
    return pl.pallas_call(
        finish_kernel,
        out_shape=(jax.ShapeDtypeStruct(shape, BF), row, row),
        in_specs=[vmem] * 3,
        out_specs=(pl.BlockSpec(memory_space=pltpu.HBM), vmem, vmem),
        scratch_shapes=[pltpu.VMEM(shape, BF), pltpu.SemaphoreType.DMA((10,))],
        compiler_params=pltpu.CompilerParams(vmem_limit_bytes=FINISH_LIMIT),
    )(sums, sigma, weighted)


def exchange(value):
    return lax.all_to_all(value, ALL, split_axis=0, concat_axis=0, tiled=True)


def local(amplitudes, virtual_fock_block, metric, active_block):
    acts = lax.axis_size("act")
    x = jnp.transpose(amplitudes, (1, 0, 2))
    rows, pairs, width = x.shape
    items = width // LANES
    packed, wide = pack(x, metric, active_block, acts)
    arrived = exchange(packed)
    sent = middle(arrived, virtual_fock_block, wide, acts, rows, pairs, items)
    sigma, weighted, partial = last(exchange(sent), x, virtual_fock_block)
    resid, rayleigh, norm = finish(exchange(partial), sigma, weighted, x.shape)
    return jnp.transpose(resid, (1, 0, 2)), rayleigh[0, 0], norm[0, 0]


def solution(mesh):
    acts, virts = mesh.shape["act"], mesh.shape["virt"]
    torus = Mesh(mesh.devices.reshape(acts, 4, virts // 8, 2), ("act",) + VIRT)
    in_specs = (P("act", VIRT, None), P(), P(), P())
    out_specs = (P("act", VIRT, None), P(), P())
    return jax.shard_map(local, mesh=torus, in_specs=in_specs, out_specs=out_specs, check_vma=False)
```
